32 devices in a mesh: seq: 4 (over z), head: 4 (over y, x), batch: 2 (over core).
Axes of the slice: x: 2, y: 2, z: 4, core: 2. Of those that a mesh axis runs over, the one named last changes fastest.
Arguments:
- ssm_input: bfloat16 [16384, 5120], P(('batch', 'seq'), 'head'), parts along dimension 0, may hold values from -500 to 500
- gate_input: bfloat16 [16384, 5120], P(('batch', 'seq'), 'head'), parts along dimension 0, may hold values from -6 to 6
- b_proj: bfloat16 [16384, 1024], P(('batch', 'seq')), parts along dimension 0, may hold values from -2 to 2
- c_proj: bfloat16 [16384, 1024], P(('batch', 'seq')), parts along dimension 0, may hold values from -2 to 2
- step_size: float32 [80, 16384], P('head', ('batch', 'seq')), parts along dimension 1, may hold values from 0.02 to 0.2
- log_decay: float32 [80, 16384], P('head', ('batch', 'seq')), parts along dimension 1, may hold values from -1.5 to 0, as said below
- skip_gain: float32 [80], P('head'), may hold values from 0.5 to 1.5
- norm_gain: float32 [5120], replicated, may hold values from 0.1 to 1.9
- out_weight: bfloat16 [5120, 2560], P('head'), may hold values from -0.078125 to 0.078125
Outputs:
- layer_out: bfloat16 [16384, 2560], P(('batch', 'seq', 'head')), parts along dimension 0
The draws below stay inside these ranges and needn't reach their ends.
There are 2 independent parts, one for each index of `batch`. The reference program is written for one: setup_inputs(seed, part) draws one part's arguments, and reference() takes and returns one part's arrays. A program takes and returns all parts, laid end to end along the dimension named above; an argument that names none is the same for every part. Nothing has to cross between parts.
Inputs may be any that keep to these rules, and one draw needn't show every extreme that they name: `log_decay`: negative.
All inputs are finite; a program needn't handle non-finite values.
Results may differ from the reference program's by a relative error of at most 0.018.
Values may be sent and summed in bfloat16 or wider, within the bound.
A program may use at most 192 MiB of HBM per device.

```python
import math
import jax
import jax.numpy as jnp
from jax import lax

D = 2560
HEAD_COUNT = 80
HEAD_DIM = 64
STATE = 128
GROUPS = 8
BLOCK = 256
SEQUENCE_LENGTH = 8192


def draw_ssm_input(key, part):
    random_keys = jax.random.split(key, 3)
    total_width = HEAD_COUNT * HEAD_DIM
    columns = 10.0 ** (jnp.arange(total_width, dtype=jnp.float32) / total_width)
    row_scale = 10.0 ** jax.random.uniform(random_keys[0], (SEQUENCE_LENGTH, 1), jnp.float32)
    values = jnp.clip(jax.random.normal(random_keys[2], (SEQUENCE_LENGTH, total_width), jnp.float32), -4.0, 4.0)
    return (values * columns[None, :] * row_scale).astype(jnp.bfloat16)


def draw_log_decay(key, part):
    random_keys = jax.random.split(key, 6)
    fast_share = 0.5
    is_fast = jax.random.uniform(random_keys[0], (HEAD_COUNT, 1), jnp.float32) < fast_share
    fast_rate = 10.0 ** jax.random.uniform(random_keys[1], (HEAD_COUNT, 1), jnp.float32, -1.699, -1.347)
    slow_rate = 10.0 ** jax.random.uniform(random_keys[2], (HEAD_COUNT, 1), jnp.float32, -1.0, 0.0) / SEQUENCE_LENGTH
    per_head_decay = jnp.where(is_fast, fast_rate, slow_rate)
    jitter_level = jax.random.uniform(random_keys[3], (HEAD_COUNT, SEQUENCE_LENGTH), jnp.float32, 0.2, 1.6)
    spike_position = jax.random.randint(random_keys[4], (2, 1), 0, SEQUENCE_LENGTH)
    spike_decay = jax.random.uniform(random_keys[5], (HEAD_COUNT, 2), jnp.float32, 0.22, 0.69)
    spike_count = (jnp.arange(SEQUENCE_LENGTH)[None, :] == spike_position).astype(jnp.float32)
    return -per_head_decay * jitter_level - jnp.dot(spike_decay, spike_count)


def shard_levels(key, dims, shards, smallest, high):
    def one(dim, shards_of):
        steps = jax.random.uniform(jax.random.fold_in(jax.random.fold_in(key, 6), dim), (shards_of,), jnp.float32, smallest / len(shards), high / len(shards))
        return jnp.repeat(jnp.exp(steps), dims[dim] // shards_of).reshape((-1,) + (1,) * (len(dims) - dim - 1))

    loudness = one(*shards[0])
    for cut in shards[1:]:
        loudness = loudness * one(*cut)
    return loudness


def gaussian(key, dims, deviation, bound, shards=(), held_as=jnp.bfloat16):
    drawn = jax.random.normal(key, dims, jnp.float32) * deviation
    if len(shards) > 0:
        drawn = shard_levels(key, dims, shards, -0.22, 0.18) * drawn
    return jnp.clip(drawn, min=-bound, max=bound).astype(held_as)


def setup_inputs(seed: int = 0, part: int = 0) -> dict:
    key_list = jax.random.split(jax.random.key(seed), 10)
    part_keys = jax.random.split(jax.random.fold_in(key_list[9], part), 10)
    return {
        "ssm_input": draw_ssm_input(jax.random.fold_in(jax.random.fold_in(key_list[9], part), 71), part),
        "gate_input": gaussian(part_keys[1], (SEQUENCE_LENGTH, HEAD_COUNT * HEAD_DIM), 1.5, 6.0, ((0, 4), (1, 4))),
        "b_proj": gaussian(part_keys[2], (SEQUENCE_LENGTH, GROUPS * STATE), 0.3, 2.0, ((0, 4),)),
        "c_proj": gaussian(part_keys[3], (SEQUENCE_LENGTH, GROUPS * STATE), 0.3, 2.0, ((0, 4),)),
        "step_size": jnp.clip(jnp.exp(math.log(0.2) - 2.3025851 * jax.random.uniform(part_keys[4], (HEAD_COUNT, SEQUENCE_LENGTH), jnp.float32) ** shard_levels(part_keys[4], (HEAD_COUNT, SEQUENCE_LENGTH), ((0, 4), (1, 4)), -0.2, 0.2)), 0.02, 0.2),
        "log_decay": draw_log_decay(jax.random.fold_in(jax.random.fold_in(key_list[9], part), 71), part),
        "skip_gain": jnp.clip(0.5 + 1.0 * jax.random.uniform(key_list[6], (HEAD_COUNT,), jnp.float32) ** shard_levels(key_list[6], (HEAD_COUNT,), ((0, 4),), -0.2, 0.2), 0.5, 1.5),
        "norm_gain": jnp.clip(1.0 + 0.18 * jax.random.normal(key_list[7], (HEAD_COUNT * HEAD_DIM,), jnp.float32), 0.1, 1.9),
        "out_weight": gaussian(key_list[8], (HEAD_COUNT * HEAD_DIM, D), (HEAD_COUNT * HEAD_DIM) ** -0.5, 0.078125, ((0, 4),)),
    }


epsilon = 1e-05

def reference(ssm_input, gate_input, b_proj, c_proj, step_size, log_decay, skip_gain, norm_gain, out_weight):
    nblocks = SEQUENCE_LENGTH // BLOCK
    group_of = jnp.arange(HEAD_COUNT) // (HEAD_COUNT // GROUPS)
    lower_mask = jnp.tril(jnp.ones((BLOCK, BLOCK), dtype=bool))

    def block_step(carried, inputs_now):
        x_block, b_block, c_block, step_block, decay_block = inputs_now
        cumulative = jnp.cumsum(decay_block, axis=1)
        b_heads = b_block.reshape(BLOCK, GROUPS, STATE)[:, group_of, :].astype(jnp.float32)
        c_heads = c_block.reshape(BLOCK, GROUPS, STATE)[:, group_of, :].astype(jnp.float32)
        scores = jnp.einsum('thn,shn->hts', c_heads, b_heads)
        differ = cumulative[:, :, None] - cumulative[:, None, :]
        weights = scores * jnp.exp(jnp.where(lower_mask, differ, -jnp.inf)) * step_block[:, None, :]
        weights = lax.optimization_barrier(weights.astype(jnp.bfloat16)).astype(jnp.float32)
        x_heads = x_block.reshape(BLOCK, HEAD_COUNT, HEAD_DIM).astype(jnp.float32)
        within = jnp.einsum('hts,shp->thp', weights, x_heads)
        entering_b = lax.optimization_barrier(carried.astype(jnp.bfloat16)).astype(jnp.float32)
        across = jnp.einsum('thn,hpn->thp', c_heads, entering_b) * jnp.exp(cumulative).T[:, :, None]
        to_end = (jnp.exp(cumulative[:, -1:] - cumulative) * step_block).T
        scaled = lax.optimization_barrier((b_heads * to_end[:, :, None]).astype(jnp.bfloat16)).astype(jnp.float32)
        block_state = jnp.einsum('shp,shn->hpn', x_heads, scaled)
        renewed = jnp.exp(cumulative[:, -1])[:, None, None] * carried + block_state
        output = within + across + skip_gain[None, :, None] * x_heads
        return (renewed, output)
    x_blocks = ssm_input.reshape(nblocks, BLOCK, HEAD_COUNT * HEAD_DIM)
    b_blocks = b_proj.reshape(nblocks, BLOCK, GROUPS * STATE)
    c_blocks = c_proj.reshape(nblocks, BLOCK, GROUPS * STATE)
    step_blocks = step_size.reshape(HEAD_COUNT, nblocks, BLOCK).transpose(1, 0, 2)
    decay_blocks = log_decay.reshape(HEAD_COUNT, nblocks, BLOCK).transpose(1, 0, 2)
    start_state = jnp.zeros((HEAD_COUNT, HEAD_DIM, STATE), jnp.float32)
    unused, outputs = lax.scan(block_step, start_state, (x_blocks, b_blocks, c_blocks, step_blocks, decay_blocks))
    output = outputs.reshape(SEQUENCE_LENGTH, HEAD_COUNT * HEAD_DIM)
    gated_rows = output * jax.nn.silu(gate_input.astype(jnp.float32))
    squares = lax.optimization_barrier(jnp.sum(gated_rows * gated_rows, axis=1, keepdims=True))
    normed = (gated_rows * lax.rsqrt(squares / (HEAD_COUNT * HEAD_DIM) + epsilon) * norm_gain).astype(jnp.bfloat16)
    return jnp.dot(normed, out_weight, preferred_element_type=jnp.float32).astype(jnp.bfloat16)
```

```python
import functools
import jax
import jax.numpy as jnp
from jax import lax
from jax.experimental import pallas as pl
from jax.experimental.pallas import tpu as pltpu
from jax.sharding import PartitionSpec as P

HEAD_COUNT = 80
HEAD_DIM = 64
STATE = 128
GROUPS = 8
BLOCK = 256
LANES = 128
UNIT = 128
epsilon = 1e-05
HIGHEST = lax.Precision.HIGHEST
F32 = jnp.float32
BF16 = jnp.bfloat16
MESH = pl.DeviceIdType.MESH


def dot(a, b, ca, cb, precision=None):
    return lax.dot_general(
        a, b, (((ca,), (cb,)), ((), ())), precision=precision, preferred_element_type=F32
    )


def iotas(rows, columns):
    return (
        lax.broadcasted_iota(jnp.int32, (rows, columns), 0),
        lax.broadcasted_iota(jnp.int32, (rows, columns), 1),
    )


def pieces(channels, repeats):
    found = []
    for start in range(0, channels, LANES):
        width = min(LANES, channels - start)
        heads = [start // HEAD_DIM + i for i in range(width // HEAD_DIM)]
        found.append((len(found), start, width, heads, heads[0] // repeats))
    return found


def spread(columns, heads, width):
    rows = columns.shape[0]
    first = jnp.broadcast_to(columns[:, heads[0] : heads[0] + 1], (rows, width))
    if len(heads) == 1:
        return first
    second = jnp.broadcast_to(columns[:, heads[1] : heads[1] + 1], (rows, width))
    lane = iotas(rows, width)[1]
    return jnp.where(lane < HEAD_DIM, first, second)


def split(value, count):
    parts = []
    for _ in range(count):
        part = value.astype(BF16)
        parts.append(part)
        value = value - part.astype(F32)
    return parts


def column_tiles(start, stop, size):
    return [(at, min(size, stop - at)) for at in range(start, stop, size)]


def mixer_kernel(
    plan, x_hbm, gate_hbm, b_hbm, c_hbm, step_hbm, log_hbm, skip_ref, gain_ref, w_hbm, out_hbm,
    x, gate, b, c, step, log, w, stack, stack2, rows_ref, cols_ref, wcols_ref, prefix, base,
    state_out, state_in, g_ref, part, squares, squares_in, first_a, first_b, second_a, second_b, stage,
    load_sem, out_sem, state_send, state_recv, square_send, square_recv,
    first_a_send, first_a_recv, first_b_send, first_b_recv,
    second_a_send, second_a_recv, second_b_send, second_b_recv,
):
    X, Y, S, groups, repeats = plan
    H = X * Y
    tokens, channels = x.shape
    model = w.shape[1]
    half = model // 2
    heads = step.shape[0]
    padded = stack.shape[0] // (tokens // BLOCK)
    blocks = tokens // BLOCK
    per_share = tokens // H
    unit = min(UNIT, per_share)
    subs = per_share // unit
    units = BLOCK // unit
    per_group = HEAD_COUNT // GROUPS
    every = pieces(channels, repeats)

    me = lax.axis_index("head")
    z = lax.axis_index("seq")
    gx = me % X
    gy = me // X
    to = lambda dx, dy: {"head": ((gy + dy) % Y) * X + (gx + dx) % X}
    after = {"seq": lax.rem(z + 1, S)}

    offset = pl.multiple_of((me * heads // per_group) // groups * (groups * STATE), STATE)
    loads = [
        pltpu.make_async_copy(log_hbm, log, load_sem.at[0]),
        pltpu.make_async_copy(step_hbm, step, load_sem.at[1]),
        pltpu.make_async_copy(b_hbm.at[:, pl.ds(offset, groups * STATE)], b, load_sem.at[2]),
        pltpu.make_async_copy(x_hbm, x, load_sem.at[3]),
        pltpu.make_async_copy(c_hbm.at[:, pl.ds(offset, groups * STATE)], c, load_sem.at[4]),
        pltpu.make_async_copy(gate_hbm, gate, load_sem.at[5]),
        pltpu.make_async_copy(w_hbm, w, load_sem.at[6]),
    ]
    for load in loads:
        load.start()

    barrier = pltpu.get_barrier_semaphore()
    for d in range(1, H):
        pl.semaphore_signal(barrier, inc=1, device_id={"head": lax.rem(me + d, H)}, device_id_type=MESH)
    if S > 1:
        @pl.when(z > 0)
        def _():
            pl.semaphore_signal(barrier, inc=1, device_id={"seq": lax.max(z - 1, 0)}, device_id_type=MESH)

        @pl.when(z < S - 1)
        def _():
            pl.semaphore_signal(barrier, inc=1, device_id=after, device_id_type=MESH)

    near = 0
    if S > 1:
        near = jnp.where(z > 0, 1, 0) + jnp.where(z < S - 1, 1, 0)
    pl.semaphore_wait(barrier, near + (H - 1))

    def state_copy(p):
        return pltpu.make_async_remote_copy(
            src_ref=state_out.at[p], dst_ref=state_in.at[p], send_sem=state_send.at[p],
            recv_sem=state_recv.at[p], device_id=after, device_id_type=MESH,
        )

    t_iota, s_iota = iotas(BLOCK, BLOCK)
    lower = jnp.where(s_iota <= t_iota, 1.0, 0.0)
    lower_b = lower.astype(BF16)
    same_b = jnp.where(s_iota == t_iota, 1.0, 0.0).astype(BF16)
    stack[...] = jnp.zeros_like(stack)
    stack2[...] = jnp.ones_like(stack2)
    prefix[0] = jnp.zeros(prefix.shape[1:], F32)
    base[0:8] = jnp.zeros((8, channels), F32)
    state_out[...] = jnp.zeros_like(state_out)

    @pl.when(z == 0)
    def _():
        state_in[...] = jnp.zeros_like(state_in)

    loads[0].wait()
    loads[1].wait()
    for k in range(blocks):
        stack[k * padded : k * padded + heads, :] = log[:, k * BLOCK : (k + 1) * BLOCK]
        stack2[k * padded : k * padded + heads, :] = step[:, k * BLOCK : (k + 1) * BLOCK]
    rows_all, cols_all = 0.0, 0.0
    for part_of in split(stack[...], 3):
        rows_all = rows_all + dot(part_of, lower_b, 1, 1)
        cols_all = cols_all + dot(lower_b, part_of, 1, 1)
    steps = stack2[...]
    rows_ref[...] = rows_all - jnp.log(steps)
    to_end = jnp.exp(rows_all[:, BLOCK - 1 : BLOCK] - rows_all) * steps
    to_end_cols = 0.0
    for part_of in split(to_end, 2):
        to_end_cols = to_end_cols + dot(same_b, part_of, 1, 1)
    for k in range(blocks):
        cols_ref[k] = cols_all[:, k * padded : (k + 1) * padded]
        wcols_ref[k] = to_end_cols[:, k * padded : (k + 1) * padded]

    loads[2].wait()
    loads[3].wait()
    middle = (len(every) + 1) // 2
    for some in (every[:middle], every[middle:]):
        if not some:
            continue

        def state_step(k, carry, some=some):
            row = pl.ds(pl.multiple_of(k * BLOCK, BLOCK), BLOCK)
            spot = pl.ds(pl.multiple_of(k * 8, 8), 8)
            following = pl.ds(pl.multiple_of(k * 8 + 8, 8), 8)
            end = cols_ref[k, BLOCK - 8 : BLOCK, :][7:8, :]
            wide = wcols_ref[k]
            for p, start, width, of, group in some:
                lanes = slice(start, start + width)
                last = spread(end, of, width)
                weighted = (x[row, lanes].astype(F32) * spread(wide, of, width)).astype(BF16)
                new = dot(b[row, group * STATE : (group + 1) * STATE], weighted, 0, 0)
                prefix[k + 1, :, lanes] = jnp.exp(last) * prefix[k, :, lanes] + new
                base[following, lanes] = base[spot, lanes] + last
            return carry

        lax.fori_loop(0, blocks, state_step, 0)
        if S > 1:
            @pl.when(z == 0)
            def _(some=some):
                for p, start, width, of, group in some:
                    state_out[p, :, :width] = prefix[blocks, :, start : start + width].astype(BF16)
                    state_copy(p).start()

    def pass_state():
        for p, start, width, of, group in every:
            lanes = slice(start, start + width)
            state_copy(p).wait_recv()

            @pl.when(z < S - 1)
            def _():
                grown = jnp.exp(base[blocks * 8 : blocks * 8 + 1, lanes]) * state_in[p, :, :width].astype(F32)
                state_out[p, :, :width] = (grown + prefix[blocks, :, lanes]).astype(BF16)
                state_copy(p).start()

    def block_of(j):
        if per_share < BLOCK:
            return j
        chunks = per_share // BLOCK
        o = j // chunks
        dx = X - 1 - o // Y
        dy = Y - 1 - o % Y
        return (((gy + dy) % Y) * X + (gx + dx) % X) * chunks + j % chunks

    def within(j):
        k = block_of(j)
        row = pl.ds(pl.multiple_of(k * BLOCK, BLOCK), BLOCK)
        mid = BLOCK // 2
        columns = cols_ref[k]
        rows = rows_ref[pl.ds(pl.multiple_of(k * padded, padded), padded), :]
        scores = {}
        for p, start, width, of, group in every:
            lanes = slice(start, start + width)
            if group not in scores:
                which = slice(group * STATE, (group + 1) * STATE)
                scores[group] = dot(c[row, which], b[row, which], 1, 1) * lower
            x_here = x[row, lanes]
            lane = iotas(BLOCK, width)[1]
            top, bottom = 0.0, 0.0
            for i, head in enumerate(of):
                kept = (lane >= i * HEAD_DIM) & (lane < (i + 1) * HEAD_DIM)
                x_head = x_here if len(of) == 1 else jnp.where(kept, x_here, jnp.zeros_like(x_here))
                column, across = columns[:, head : head + 1], rows[head : head + 1, :]
                w_top = scores[group][:mid, :mid] * jnp.exp(
                    jnp.minimum(column[:mid] - across[:, :mid], 0.0)
                )
                w_bottom = scores[group][mid:] * jnp.exp(jnp.minimum(column[mid:] - across, 0.0))
                top = top + dot(w_top.astype(BF16), x_head[:mid], 1, 0)
                bottom = bottom + dot(w_bottom.astype(BF16), x_head, 1, 0)
            direct = skip_ref[:, lanes] * x_here.astype(F32)
            x[row, lanes] = jnp.concatenate([top + direct[:mid], bottom + direct[mid:]], axis=0).astype(BF16)

    def first_copy(buffer, send, recv, dx, dy, sub, row, columns, slot):
        return pltpu.make_async_remote_copy(
            src_ref=part.at[pl.ds(row, unit), columns],
            dst_ref=buffer.at[slot[0], slot[1], sub],
            send_sem=send.at[slot[0], slot[1], sub],
            recv_sem=recv.at[slot[0], slot[1], sub],
            device_id=to(dx, dy), device_id_type=MESH,
        )

    def copy_a(dx, dy, sub, row):
        return first_copy(
            first_a, first_a_send, first_a_recv, dx, 0, sub, row, pl.ds(0, half), (dx - 1, dy)
        )

    def copy_b(dx, dy, sub, row):
        return first_copy(
            first_b, first_b_send, first_b_recv, 0, dy, sub, row, pl.ds(half, model - half), (dy - 1, dx)
        )

    def copy_squares(dx, dy, sub, index):
        slot = dx * Y + dy
        return pltpu.make_async_remote_copy(
            src_ref=squares.at[index], dst_ref=squares_in.at[slot, sub],
            send_sem=square_send.at[slot, sub], recv_sem=square_recv.at[slot, sub],
            device_id=to(dx, dy), device_id_type=MESH,
        )

    def finish(j):
        k = block_of(j)
        row = pl.ds(pl.multiple_of(k * BLOCK, BLOCK), BLOCK)
        grow_all = jnp.exp(cols_ref[k])
        before = jnp.exp(base[pl.ds(pl.multiple_of(k * 8, 8), 8), :])
        total = {}
        for p, start, width, of, group in every:
            lanes = slice(start, start + width)
            entering = prefix[k, :, lanes] + before[0:1, lanes] * state_in[p, :, :width].astype(F32)
            moved = dot(c[row, group * STATE : (group + 1) * STATE], entering.astype(BF16), 1, 0)
            across = spread(grow_all, of, width) * moved
            v = gate[row, lanes].astype(F32)
            gated = (x[row, lanes].astype(F32) + across) * (v * (0.5 + 0.5 * jnp.tanh(0.5 * v)))
            total[width] = total.get(width, 0.0) + gated * gated
            g_ref[:, lanes] = (gated * gain_ref[:, lanes]).astype(BF16)
        summed = jnp.zeros((8, BLOCK), F32)
        for width, value in total.items():
            for part_of in split(value, 2):
                summed = summed + dot(jnp.ones((8, width), BF16), part_of, 1, 1)
        for u in range(units):
            squares[k * units + u] = summed[:, u * unit : (u + 1) * unit]
        where = []
        for u in range(units):
            begin = pl.multiple_of(k * BLOCK + u * unit, unit)
            owner = begin // per_share
            sub = (begin % per_share) // unit
            where.append(((owner % X - gx + X) % X, (owner // X - gy + Y) % Y, sub, begin, k * units + u))
        for start, width in column_tiles(0, half, 512):
            part[row, start : start + width] = dot(g_ref[...], w[:, start : start + width], 1, 0).astype(BF16)
        for dx, dy, sub, begin, index in where:
            @pl.when(dx > 0)
            def _():
                copy_a(dx, dy, sub, begin).start()
        for start, width in column_tiles(half, model, 512):
            part[row, start : start + width] = dot(g_ref[...], w[:, start : start + width], 1, 0).astype(BF16)
        for dx, dy, sub, begin, index in where:
            @pl.when(dy > 0)
            def _():
                copy_b(dx, dy, sub, begin).start()

            @pl.when(dx + dy > 0)
            def _():
                copy_squares(dx, dy, sub, index).start()

    loads[4].wait()
    lag = max(1, (S - 1) * blocks // S) if S > 1 else 1
    waits = jnp.where(z > 0, lax.max(z * blocks // S, 1) - 1, -1) if S > 1 else None

    def main_step(i, carry):
        @pl.when(i < blocks)
        def _():
            within(i)

        if S > 1:
            @pl.when(i == waits)
            def _():
                pass_state()

        @pl.when(i == lag)
        def _():
            loads[5].wait()
            loads[6].wait()

        @pl.when(i >= lag)
        def _():
            finish(i - lag)

        return carry

    lax.fori_loop(0, blocks + lag, main_step, 0)

    def second_copy(buffer, send, recv, dx, dy, slot, sub, row, columns):
        return pltpu.make_async_remote_copy(
            src_ref=part.at[pl.ds(row, unit), columns], dst_ref=buffer.at[slot, sub],
            send_sem=send.at[slot, sub], recv_sem=recv.at[slot, sub],
            device_id=to(dx, dy), device_id_type=MESH,
        )

    left, right = pl.ds(0, half), pl.ds(half, model - half)

    def row_of(dx, dy, sub):
        owner = ((gy + dy) % Y) * X + (gx + dx) % X
        return pl.multiple_of(owner * per_share + sub * unit, unit)

    second_a_copy = lambda dy, sub: second_copy(
        second_a, second_a_send, second_a_recv, 0, dy, dy - 1, sub, row_of(0, dy, sub), left
    )
    second_b_copy = lambda dx, sub: second_copy(
        second_b, second_b_send, second_b_recv, dx, 0, dx - 1, sub, row_of(dx, 0, sub), right
    )

    def partial_sum(row, columns, buffer, copy, count, other, sub):
        value = part[pl.ds(row, unit), columns].astype(F32)
        for d in range(1, count):
            copy(d, other, sub, row).wait_recv()
            value = value + buffer[d - 1, other, sub].astype(F32)
        return value

    swapped_b = lambda dy, dx, sub, row: copy_b(dx, dy, sub, row)

    def relay(sub, carry):
        for dy in range(1, Y):
            row = row_of(0, dy, sub)
            part[pl.ds(row, unit), left] = partial_sum(row, left, first_a, copy_a, X, dy, sub).astype(BF16)
            second_a_copy(dy, sub).start()
        for dx in range(1, X):
            row = row_of(dx, 0, sub)
            part[pl.ds(row, unit), right] = partial_sum(row, right, first_b, swapped_b, Y, dx, sub).astype(BF16)
            second_b_copy(dx, sub).start()
        return carry

    lax.fori_loop(0, subs, relay, 0)

    def out_copy(sub):
        there = pl.ds(pl.multiple_of(sub * unit, unit), unit)
        return pltpu.make_async_copy(stage.at[there, :], out_hbm.at[there, :], out_sem.at[sub])

    same_u = jnp.where(iotas(unit, unit)[0] == iotas(unit, unit)[1], 1.0, 0.0)

    def settle(sub, carry):
        row = row_of(0, 0, sub)
        there = pl.ds(pl.multiple_of(sub * unit, unit), unit)
        summed = squares[me * subs + sub]
        for dx in range(X):
            for dy in range(Y):
                if dx + dy > 0:
                    copy_squares(dx, dy, sub, 0).wait_recv()
                    summed = summed + squares_in[dx * Y + dy, sub]
        column = dot(same_u, summed, 1, 1, HIGHEST)[:, 0:1]
        scale = lax.rsqrt(column / (HEAD_COUNT * HEAD_DIM) + epsilon)
        value = partial_sum(row, left, first_a, copy_a, X, 0, sub)
        for dy in range(1, Y):
            second_a_copy(dy, sub).wait_recv()
            value = value + second_a[dy - 1, sub].astype(F32)
        stage[there, left] = (value * scale).astype(BF16)
        value = partial_sum(row, right, first_b, swapped_b, Y, 0, sub)
        for dx in range(1, X):
            second_b_copy(dx, sub).wait_recv()
            value = value + second_b[dx - 1, sub].astype(F32)
        stage[there, right] = (value * scale).astype(BF16)
        out_copy(sub).start()
        return carry

    lax.fori_loop(0, subs, settle, 0)

    def drain(sub, carry):
        for dx in range(X):
            for dy in range(Y):
                if dx > 0:
                    copy_a(dx, dy, sub, 0).wait_send()
                if dy > 0:
                    copy_b(dx, dy, sub, 0).wait_send()
                if dx + dy > 0:
                    copy_squares(dx, dy, sub, 0).wait_send()
        for dy in range(1, Y):
            second_a_copy(dy, sub).wait_send()
        for dx in range(1, X):
            second_b_copy(dx, sub).wait_send()
        out_copy(sub).wait()
        return carry

    lax.fori_loop(0, subs, drain, 0)
    if S > 1:
        @pl.when(z < S - 1)
        def _():
            for p, start, width, of, group in every:
                state_copy(p).wait_send()


def body(
    ssm_input, gate_input, b_proj, c_proj, step_size, log_decay, skip_gain, norm_gain, out_weight
):
    tokens, channels = ssm_input.shape
    heads = step_size.shape[0]
    blocks = tokens // BLOCK
    model = out_weight.shape[1]
    half = model // 2
    per_group = HEAD_COUNT // GROUPS
    groups = max(1, heads // per_group)
    repeats = min(heads, per_group)
    H = lax.axis_size("head")
    S = lax.axis_size("seq")
    X = max(d for d in range(1, H + 1) if H % d == 0 and d * d <= H)
    Y = H // X
    per_share = tokens // H
    unit = min(UNIT, per_share)
    subs = per_share // unit
    count = len(pieces(channels, repeats))
    padded = -(-heads // 8) * 8
    head_index = lax.axis_index("head")
    skip = jnp.repeat(skip_gain, HEAD_DIM)[None, :]
    gain = lax.dynamic_slice_in_dim(norm_gain, head_index * channels, channels)[None, :]
    anywhere = pl.BlockSpec(memory_space=pl.ANY)
    vmem = pl.BlockSpec(memory_space=pltpu.VMEM)
    dma = pltpu.SemaphoreType.DMA
    x1, y1 = max(X - 1, 1), max(Y - 1, 1)
    return pl.pallas_call(
        functools.partial(mixer_kernel, (X, Y, S, groups, repeats)),
        in_specs=[anywhere] * 6 + [vmem, vmem, anywhere],
        out_specs=anywhere,
        out_shape=jax.ShapeDtypeStruct((per_share, model), BF16),
        scratch_shapes=[
            pltpu.VMEM((tokens, channels), BF16),
            pltpu.VMEM((tokens, channels), BF16),
            pltpu.VMEM((tokens, groups * STATE), BF16),
            pltpu.VMEM((tokens, groups * STATE), BF16),
            pltpu.VMEM((heads, tokens), F32),
            pltpu.VMEM((heads, tokens), F32),
            pltpu.VMEM((channels, model), BF16),
            pltpu.VMEM((blocks * padded, BLOCK), F32),
            pltpu.VMEM((blocks * padded, BLOCK), F32),
            pltpu.VMEM((blocks * padded, BLOCK), F32),
            pltpu.VMEM((blocks, BLOCK, padded), F32),
            pltpu.VMEM((blocks, BLOCK, padded), F32),
            pltpu.VMEM((blocks + 1, STATE, channels), F32),
            pltpu.VMEM(((blocks + 1) * 8, channels), F32),
            pltpu.VMEM((count, STATE, LANES), BF16),
            pltpu.VMEM((count, STATE, LANES), BF16),
            pltpu.VMEM((BLOCK, channels), BF16),
            pltpu.VMEM((tokens, model), BF16),
            pltpu.VMEM((tokens // unit, 8, unit), F32),
            pltpu.VMEM((H, subs, 8, unit), F32),
            pltpu.VMEM((x1, Y, subs, unit, half), BF16),
            pltpu.VMEM((y1, X, subs, unit, model - half), BF16),
            pltpu.VMEM((y1, subs, unit, half), BF16),
            pltpu.VMEM((x1, subs, unit, model - half), BF16),
            pltpu.VMEM((per_share, model), BF16),
            dma((7,)),
            dma((subs,)),
            dma((count,)),
            dma((count,)),
            dma((H, subs)),
            dma((H, subs)),
            dma((x1, Y, subs)),
            dma((x1, Y, subs)),
            dma((y1, X, subs)),
            dma((y1, X, subs)),
            dma((y1, subs)),
            dma((y1, subs)),
            dma((x1, subs)),
            dma((x1, subs)),
        ],
        compiler_params=pltpu.CompilerParams(
            collective_id=0, has_side_effects=True, vmem_limit_bytes=62 * 1024 * 1024
        ),
        name="mixer",
        cost_estimate=pl.CostEstimate(
            flops=2 * tokens * channels * (model + 4 * BLOCK), bytes_accessed=tokens * channels * 8, transcendentals=0
        ),
    )(ssm_input, gate_input, b_proj, c_proj, step_size, log_decay, skip, gain, out_weight)


def solution(mesh):
    in_specs = (
        P(("batch", "seq"), "head"),
        P(("batch", "seq"), "head"),
        P(("batch", "seq"), None),
        P(("batch", "seq"), None),
        P("head", ("batch", "seq")),
        P("head", ("batch", "seq")),
        P("head"),
        P(),
        P("head", None),
    )
    out_specs = P(("batch", "seq", "head"), None)
    return jax.shard_map(body, mesh=mesh, in_specs=in_specs, out_specs=out_specs, check_vma=False)
```

```python
import functools
import jax
import jax.numpy as jnp
from jax import lax
from jax.experimental import pallas as pl
from jax.experimental.pallas import tpu as pltpu
from jax.sharding import PartitionSpec as P

HEAD_COUNT = 80
HEAD_DIM = 64
STATE = 128
GROUPS = 8
BLOCK = 256
LANES = 128
UNIT = 128
epsilon = 1e-05
HIGHEST = lax.Precision.HIGHEST
F32 = jnp.float32
BF16 = jnp.bfloat16
MESH = pl.DeviceIdType.MESH


def dot(a, b, ca, cb, precision=None):
    return lax.dot_general(
        a, b, (((ca,), (cb,)), ((), ())), precision=precision, preferred_element_type=F32
    )


def iotas(rows, columns):
    return (
        lax.broadcasted_iota(jnp.int32, (rows, columns), 0),
        lax.broadcasted_iota(jnp.int32, (rows, columns), 1),
    )


def pieces(channels, repeats):
    found = []
    for start in range(0, channels, LANES):
        width = min(LANES, channels - start)
        heads = [start // HEAD_DIM + i for i in range(width // HEAD_DIM)]
        found.append((len(found), start, width, heads, heads[0] // repeats))
    return found


def spread(columns, heads, width):
    rows = columns.shape[0]
    first = jnp.broadcast_to(columns[:, heads[0] : heads[0] + 1], (rows, width))
    if len(heads) == 1:
        return first
    second = jnp.broadcast_to(columns[:, heads[1] : heads[1] + 1], (rows, width))
    lane = iotas(rows, width)[1]
    return jnp.where(lane < HEAD_DIM, first, second)


def split(value, count):
    parts = []
    for _ in range(count):
        part = value.astype(BF16)
        parts.append(part)
        value = value - part.astype(F32)
    return parts


def column_tiles(start, stop, size):
    return [(at, min(size, stop - at)) for at in range(start, stop, size)]


def mixer_kernel(
    plan, x_hbm, gate_hbm, b_hbm, c_hbm, step_hbm, log_hbm, skip_ref, gain_ref, w_hbm, out_hbm,
    x, gate, b, c, step, log, w, stack, stack2, rows_ref, cols_ref, ends_ref, prefix, base,
    state_out, state_in, g_ref, part, squares, squares_in, first_a, first_b, second_a, second_b, stage,
    load_sem, out_sem, state_send, state_recv, square_send, square_recv,
    first_a_send, first_a_recv, first_b_send, first_b_recv,
    second_a_send, second_a_recv, second_b_send, second_b_recv,
):
    X, Y, S, groups, repeats = plan
    H = X * Y
    tokens, channels = x.shape
    model = w.shape[1]
    half = model // 2
    heads = step.shape[0]
    padded = stack.shape[0] // (tokens // BLOCK)
    blocks = tokens // BLOCK
    per_share = tokens // H
    unit = min(UNIT, per_share)
    subs = per_share // unit
    units = BLOCK // unit
    per_group = HEAD_COUNT // GROUPS
    every = pieces(channels, repeats)
    first_gain = lax.axis_index("head") * len(every) if channels % LANES == 0 else 0

    me = lax.axis_index("head")
    z = lax.axis_index("seq")
    gx = me % X
    gy = me // X
    to = lambda dx, dy: {"head": ((gy + dy) % Y) * X + (gx + dx) % X}
    after = {"seq": lax.rem(z + 1, S)}

    offset = pl.multiple_of((me * heads // per_group) // groups * (groups * STATE), STATE)
    loads = [
        pltpu.make_async_copy(log_hbm, log, load_sem.at[0]),
        pltpu.make_async_copy(step_hbm, step, load_sem.at[1]),
        pltpu.make_async_copy(b_hbm.at[:, pl.ds(offset, groups * STATE)], b, load_sem.at[2]),
        pltpu.make_async_copy(x_hbm, x, load_sem.at[3]),
        pltpu.make_async_copy(c_hbm.at[:, pl.ds(offset, groups * STATE)], c, load_sem.at[4]),
        pltpu.make_async_copy(gate_hbm, gate, load_sem.at[5]),
        pltpu.make_async_copy(w_hbm, w, load_sem.at[6]),
    ]
    for load in loads:
        load.start()

    barrier = pltpu.get_barrier_semaphore()
    for d in range(1, H):
        pl.semaphore_signal(barrier, inc=1, device_id={"head": lax.rem(me + d, H)}, device_id_type=MESH)
    if S > 1:
        @pl.when(z > 0)
        def _():
            pl.semaphore_signal(barrier, inc=1, device_id={"seq": lax.max(z - 1, 0)}, device_id_type=MESH)

        @pl.when(z < S - 1)
        def _():
            pl.semaphore_signal(barrier, inc=1, device_id=after, device_id_type=MESH)

    near = 0
    if S > 1:
        near = jnp.where(z > 0, 1, 0) + jnp.where(z < S - 1, 1, 0)
    pl.semaphore_wait(barrier, near + (H - 1))

    def state_copy(p):
        return pltpu.make_async_remote_copy(
            src_ref=state_out.at[p], dst_ref=state_in.at[p], send_sem=state_send.at[p],
            recv_sem=state_recv.at[p], device_id=after, device_id_type=MESH,
        )

    t_iota, s_iota = iotas(BLOCK, BLOCK)
    lower = jnp.where(s_iota <= t_iota, 1.0, 0.0)
    lower_b = lower.astype(BF16)
    stack[...] = jnp.zeros_like(stack)
    stack2[...] = jnp.ones_like(stack2)
    prefix[0] = jnp.zeros(prefix.shape[1:], F32)
    base[0:8] = jnp.zeros((8, channels), F32)
    state_out[...] = jnp.zeros_like(state_out)

    @pl.when(z == 0)
    def _():
        state_in[...] = jnp.zeros_like(state_in)

    loads[0].wait()
    loads[1].wait()
    for k in range(blocks):
        stack[k * padded : k * padded + heads, :] = log[:, k * BLOCK : (k + 1) * BLOCK]
        stack2[k * padded : k * padded + heads, :] = step[:, k * BLOCK : (k + 1) * BLOCK]
    rows_all, cols_all = 0.0, 0.0
    for part_of in split(stack[...], 3):
        rows_all = rows_all + dot(part_of, lower_b, 1, 1)
        cols_all = cols_all + dot(lower_b, part_of, 1, 1)
    steps = stack2[...]
    rows_ref[...] = rows_all - jnp.log(steps)
    to_end = jnp.exp(rows_all[:, BLOCK - 1 : BLOCK] - rows_all) * steps
    ends_ref[...] = to_end
    for k in range(blocks):
        cols_ref[k] = cols_all[:, k * padded : (k + 1) * padded]

    loads[2].wait()
    loads[3].wait()
    middle = (len(every) + 1) // 2
    for some in (every[:middle], every[middle:]):
        if not some:
            continue

        def state_step(k, carry, some=some):
            row = pl.ds(pl.multiple_of(k * BLOCK, BLOCK), BLOCK)
            spot = pl.ds(pl.multiple_of(k * 8, 8), 8)
            following = pl.ds(pl.multiple_of(k * 8 + 8, 8), 8)
            end = cols_ref[k, BLOCK - 8 : BLOCK, :][7:8, :]
            ends = ends_ref[pl.ds(pl.multiple_of(k * padded, padded), padded), :]
            turned = {}
            for p, start, width, of, group in some:
                lanes = slice(start, start + width)
                last = spread(end, of, width)
                if group not in turned:
                    turned[group] = b[row, group * STATE : (group + 1) * STATE].T.astype(F32)
                scaled = [(turned[group] * ends[head : head + 1, :]).astype(BF16) for head in of]
                both = dot(jnp.concatenate(scaled, axis=0), x[row, lanes], 1, 0)
                new = both[:STATE]
                if len(of) > 1:
                    new = jnp.where(iotas(STATE, width)[1] < HEAD_DIM, new, both[STATE:])
                prefix[k + 1, :, lanes] = jnp.exp(last) * prefix[k, :, lanes] + new
                base[following, lanes] = base[spot, lanes] + last
            return carry

        lax.fori_loop(0, blocks, state_step, 0)
        if S > 1:
            @pl.when(z == 0)
            def _(some=some):
                for p, start, width, of, group in some:
                    state_out[p, :, :width] = prefix[blocks, :, start : start + width].astype(BF16)
                    state_copy(p).start()

    def pass_state():
        for p, start, width, of, group in every:
            lanes = slice(start, start + width)
            state_copy(p).wait_recv()

            @pl.when(z < S - 1)
            def _():
                grown = jnp.exp(base[blocks * 8 : blocks * 8 + 1, lanes]) * state_in[p, :, :width].astype(F32)
                state_out[p, :, :width] = (grown + prefix[blocks, :, lanes]).astype(BF16)
                state_copy(p).start()

    def block_of(j):
        if per_share < BLOCK:
            return j
        chunks = per_share // BLOCK
        o = j // chunks
        dx = X - 1 - o // Y
        dy = Y - 1 - o % Y
        return (((gy + dy) % Y) * X + (gx + dx) % X) * chunks + j % chunks

    def within(j):
        k = block_of(j)
        row = pl.ds(pl.multiple_of(k * BLOCK, BLOCK), BLOCK)
        mid = BLOCK // 2
        columns = cols_ref[k]
        rows = rows_ref[pl.ds(pl.multiple_of(k * padded, padded), padded), :]
        scores = {}
        for p, start, width, of, group in every:
            lanes = slice(start, start + width)
            if group not in scores:
                which = slice(group * STATE, (group + 1) * STATE)
                scores[group] = dot(c[row, which], b[row, which], 1, 1) * lower
            x_here = x[row, lanes]
            lane = iotas(BLOCK, width)[1]
            top, bottom = 0.0, 0.0
            for i, head in enumerate(of):
                kept = (lane >= i * HEAD_DIM) & (lane < (i + 1) * HEAD_DIM)
                x_head = x_here if len(of) == 1 else jnp.where(kept, x_here, jnp.zeros_like(x_here))
                column, across = columns[:, head : head + 1], rows[head : head + 1, :]
                w_top = scores[group][:mid, :mid] * jnp.exp(
                    jnp.minimum(column[:mid] - across[:, :mid], 0.0)
                )
                w_bottom = scores[group][mid:] * jnp.exp(jnp.minimum(column[mid:] - across, 0.0))
                top = top + dot(w_top.astype(BF16), x_head[:mid], 1, 0)
                bottom = bottom + dot(w_bottom.astype(BF16), x_head, 1, 0)
            gains = jnp.full((1, width), skip_ref[of[0]], F32)
            if len(of) > 1:
                gains = jnp.where(iotas(1, width)[1] < HEAD_DIM, gains, skip_ref[of[1]])
            direct = gains * x_here.astype(F32)
            x[row, lanes] = jnp.concatenate([top + direct[:mid], bottom + direct[mid:]], axis=0).astype(BF16)

    def first_copy(buffer, send, recv, dx, dy, sub, row, columns, slot):
        return pltpu.make_async_remote_copy(
            src_ref=part.at[pl.ds(row, unit), columns],
            dst_ref=buffer.at[slot[0], slot[1], sub],
            send_sem=send.at[slot[0], slot[1], sub],
            recv_sem=recv.at[slot[0], slot[1], sub],
            device_id=to(dx, dy), device_id_type=MESH,
        )

    def copy_a(dx, dy, sub, row):
        return first_copy(
            first_a, first_a_send, first_a_recv, dx, 0, sub, row, pl.ds(0, half), (dx - 1, dy)
        )

    def copy_b(dx, dy, sub, row):
        return first_copy(
            first_b, first_b_send, first_b_recv, 0, dy, sub, row, pl.ds(half, model - half), (dy - 1, dx)
        )

    def copy_squares(dx, dy, sub, index):
        slot = dx * Y + dy
        return pltpu.make_async_remote_copy(
            src_ref=squares.at[index], dst_ref=squares_in.at[slot, sub],
            send_sem=square_send.at[slot, sub], recv_sem=square_recv.at[slot, sub],
            device_id=to(dx, dy), device_id_type=MESH,
        )

    def finish(j):
        k = block_of(j)
        row = pl.ds(pl.multiple_of(k * BLOCK, BLOCK), BLOCK)
        grow_all = jnp.exp(cols_ref[k])
        before = jnp.exp(base[pl.ds(pl.multiple_of(k * 8, 8), 8), :])
        total = {}
        for p, start, width, of, group in every:
            lanes = slice(start, start + width)
            entering = prefix[k, :, lanes] + before[0:1, lanes] * state_in[p, :, :width].astype(F32)
            moved = dot(c[row, group * STATE : (group + 1) * STATE], entering.astype(BF16), 1, 0)
            across = spread(grow_all, of, width) * moved
            v = gate[row, lanes].astype(F32)
            gated = (x[row, lanes].astype(F32) + across) * (v * (0.5 + 0.5 * jnp.tanh(0.5 * v)))
            total[width] = total.get(width, 0.0) + gated * gated
            g_ref[:, lanes] = (gated * gain_ref[pl.ds(first_gain + p, 1), :width]).astype(BF16)
        summed = jnp.zeros((8, BLOCK), F32)
        for width, value in total.items():
            for part_of in split(value, 2):
                summed = summed + dot(jnp.ones((8, width), BF16), part_of, 1, 1)
        for u in range(units):
            squares[k * units + u] = summed[:, u * unit : (u + 1) * unit]
        where = []
        for u in range(units):
            begin = pl.multiple_of(k * BLOCK + u * unit, unit)
            owner = begin // per_share
            sub = (begin % per_share) // unit
            where.append(((owner % X - gx + X) % X, (owner // X - gy + Y) % Y, sub, begin, k * units + u))
        for start, width in column_tiles(0, half, 512):
            part[row, start : start + width] = dot(g_ref[...], w[:, start : start + width], 1, 0).astype(BF16)
        for dx, dy, sub, begin, index in where:
            @pl.when(dx > 0)
            def _():
                copy_a(dx, dy, sub, begin).start()
        for start, width in column_tiles(half, model, 512):
            part[row, start : start + width] = dot(g_ref[...], w[:, start : start + width], 1, 0).astype(BF16)
        for dx, dy, sub, begin, index in where:
            @pl.when(dy > 0)
            def _():
                copy_b(dx, dy, sub, begin).start()

            @pl.when(dx + dy > 0)
            def _():
                copy_squares(dx, dy, sub, index).start()

    loads[4].wait()
    waits = jnp.where(z > 0, lax.min(z * blocks // (S - 1), blocks - 1), -1) if S > 1 else None

    def within_step(i, carry):
        within(i)
        if S > 1:
            @pl.when(i == waits)
            def _():
                pass_state()

        return carry

    def finish_step(i, carry):
        finish(i)
        return carry

    lax.fori_loop(0, blocks, within_step, 0)
    loads[5].wait()
    loads[6].wait()
    lax.fori_loop(0, blocks, finish_step, 0)

    def second_copy(buffer, send, recv, dx, dy, slot, sub, row, columns):
        return pltpu.make_async_remote_copy(
            src_ref=part.at[pl.ds(row, unit), columns], dst_ref=buffer.at[slot, sub],
            send_sem=send.at[slot, sub], recv_sem=recv.at[slot, sub],
            device_id=to(dx, dy), device_id_type=MESH,
        )

    left, right = pl.ds(0, half), pl.ds(half, model - half)

    def row_of(dx, dy, sub):
        owner = ((gy + dy) % Y) * X + (gx + dx) % X
        return pl.multiple_of(owner * per_share + sub * unit, unit)

    second_a_copy = lambda dy, sub: second_copy(
        second_a, second_a_send, second_a_recv, 0, dy, dy - 1, sub, row_of(0, dy, sub), left
    )
    second_b_copy = lambda dx, sub: second_copy(
        second_b, second_b_send, second_b_recv, dx, 0, dx - 1, sub, row_of(dx, 0, sub), right
    )

    def partial_sum(row, columns, buffer, copy, count, other, sub):
        value = part[pl.ds(row, unit), columns].astype(F32)
        for d in range(1, count):
            copy(d, other, sub, row).wait_recv()
            value = value + buffer[d - 1, other, sub].astype(F32)
        return value

    swapped_b = lambda dy, dx, sub, row: copy_b(dx, dy, sub, row)

    def relay(sub, carry):
        for dy in range(1, Y):
            row = row_of(0, dy, sub)
            part[pl.ds(row, unit), left] = partial_sum(row, left, first_a, copy_a, X, dy, sub).astype(BF16)
            second_a_copy(dy, sub).start()
        for dx in range(1, X):
            row = row_of(dx, 0, sub)
            part[pl.ds(row, unit), right] = partial_sum(row, right, first_b, swapped_b, Y, dx, sub).astype(BF16)
            second_b_copy(dx, sub).start()
        return carry

    lax.fori_loop(0, subs, relay, 0)

    def out_copy(sub):
        there = pl.ds(pl.multiple_of(sub * unit, unit), unit)
        return pltpu.make_async_copy(stage.at[there, :], out_hbm.at[there, :], out_sem.at[sub])

    same_u = jnp.where(iotas(unit, unit)[0] == iotas(unit, unit)[1], 1.0, 0.0)

    def settle(sub, carry):
        row = row_of(0, 0, sub)
        there = pl.ds(pl.multiple_of(sub * unit, unit), unit)
        summed = squares[me * subs + sub]
        for dx in range(X):
            for dy in range(Y):
                if dx + dy > 0:
                    copy_squares(dx, dy, sub, 0).wait_recv()
                    summed = summed + squares_in[dx * Y + dy, sub]
        column = dot(same_u, summed, 1, 1, HIGHEST)[:, 0:1]
        scale = lax.rsqrt(column / (HEAD_COUNT * HEAD_DIM) + epsilon)
        value = partial_sum(row, left, first_a, copy_a, X, 0, sub)
        for dy in range(1, Y):
            second_a_copy(dy, sub).wait_recv()
            value = value + second_a[dy - 1, sub].astype(F32)
        stage[there, left] = (value * scale).astype(BF16)
        value = partial_sum(row, right, first_b, swapped_b, Y, 0, sub)
        for dx in range(1, X):
            second_b_copy(dx, sub).wait_recv()
            value = value + second_b[dx - 1, sub].astype(F32)
        stage[there, right] = (value * scale).astype(BF16)
        out_copy(sub).start()
        return carry

    lax.fori_loop(0, subs, settle, 0)

    def drain(sub, carry):
        for dx in range(X):
            for dy in range(Y):
                if dx > 0:
                    copy_a(dx, dy, sub, 0).wait_send()
                if dy > 0:
                    copy_b(dx, dy, sub, 0).wait_send()
                if dx + dy > 0:
                    copy_squares(dx, dy, sub, 0).wait_send()
        for dy in range(1, Y):
            second_a_copy(dy, sub).wait_send()
        for dx in range(1, X):
            second_b_copy(dx, sub).wait_send()
        out_copy(sub).wait()
        return carry

    lax.fori_loop(0, subs, drain, 0)
    if S > 1:
        @pl.when(z < S - 1)
        def _():
            for p, start, width, of, group in every:
                state_copy(p).wait_send()


def body(
    ssm_input, gate_input, b_proj, c_proj, step_size, log_decay, skip_gain, norm_gain, out_weight
):
    tokens, channels = ssm_input.shape
    heads = step_size.shape[0]
    blocks = tokens // BLOCK
    model = out_weight.shape[1]
    half = model // 2
    per_group = HEAD_COUNT // GROUPS
    groups = max(1, heads // per_group)
    repeats = min(heads, per_group)
    H = lax.axis_size("head")
    S = lax.axis_size("seq")
    X = max(d for d in range(1, H + 1) if H % d == 0 and d * d <= H)
    Y = H // X
    per_share = tokens // H
    unit = min(UNIT, per_share)
    subs = per_share // unit
    count = len(pieces(channels, repeats))
    padded = -(-heads // 8) * 8
    head_index = lax.axis_index("head")
    gain = norm_gain
    if channels % LANES != 0:
        gain = lax.dynamic_slice_in_dim(norm_gain, head_index * channels, channels)
        gain = jnp.pad(gain, (0, count * LANES - channels))
    gain = gain.reshape(-1, LANES)
    anywhere = pl.BlockSpec(memory_space=pl.ANY)
    vmem = pl.BlockSpec(memory_space=pltpu.VMEM)
    dma = pltpu.SemaphoreType.DMA
    x1, y1 = max(X - 1, 1), max(Y - 1, 1)
    return pl.pallas_call(
        functools.partial(mixer_kernel, (X, Y, S, groups, repeats)),
        in_specs=[anywhere] * 6 + [pl.BlockSpec(memory_space=pltpu.SMEM), vmem, anywhere],
        out_specs=anywhere,
        out_shape=jax.ShapeDtypeStruct((per_share, model), BF16),
        scratch_shapes=[
            pltpu.VMEM((tokens, channels), BF16),
            pltpu.VMEM((tokens, channels), BF16),
            pltpu.VMEM((tokens, groups * STATE), BF16),
            pltpu.VMEM((tokens, groups * STATE), BF16),
            pltpu.VMEM((heads, tokens), F32),
            pltpu.VMEM((heads, tokens), F32),
            pltpu.VMEM((channels, model), BF16),
            pltpu.VMEM((blocks * padded, BLOCK), F32),
            pltpu.VMEM((blocks * padded, BLOCK), F32),
            pltpu.VMEM((blocks * padded, BLOCK), F32),
            pltpu.VMEM((blocks, BLOCK, padded), F32),
            pltpu.VMEM((blocks * padded, BLOCK), F32),
            pltpu.VMEM((blocks + 1, STATE, channels), F32),
            pltpu.VMEM(((blocks + 1) * 8, channels), F32),
            pltpu.VMEM((count, STATE, LANES), BF16),
            pltpu.VMEM((count, STATE, LANES), BF16),
            pltpu.VMEM((BLOCK, channels), BF16),
            pltpu.VMEM((tokens, model), BF16),
            pltpu.VMEM((tokens // unit, 8, unit), F32),
            pltpu.VMEM((H, subs, 8, unit), F32),
            pltpu.VMEM((x1, Y, subs, unit, half), BF16),
            pltpu.VMEM((y1, X, subs, unit, model - half), BF16),
            pltpu.VMEM((y1, subs, unit, half), BF16),
            pltpu.VMEM((x1, subs, unit, model - half), BF16),
            pltpu.VMEM((per_share, model), BF16),
            dma((7,)),
            dma((subs,)),
            dma((count,)),
            dma((count,)),
            dma((H, subs)),
            dma((H, subs)),
            dma((x1, Y, subs)),
            dma((x1, Y, subs)),
            dma((y1, X, subs)),
            dma((y1, X, subs)),
            dma((y1, subs)),
            dma((y1, subs)),
            dma((x1, subs)),
            dma((x1, subs)),
        ],
        compiler_params=pltpu.CompilerParams(
            collective_id=0, has_side_effects=True, vmem_limit_bytes=62 * 1024 * 1024
        ),
        name="mixer",
        cost_estimate=pl.CostEstimate(
            flops=2 * tokens * channels * (model + 4 * BLOCK), bytes_accessed=tokens * channels * 8, transcendentals=0
        ),
    )(ssm_input, gate_input, b_proj, c_proj, step_size, log_decay, skip_gain, gain, out_weight)


def solution(mesh):
    in_specs = (
        P(("batch", "seq"), "head"),
        P(("batch", "seq"), "head"),
        P(("batch", "seq"), None),
        P(("batch", "seq"), None),
        P("head", ("batch", "seq")),
        P("head", ("batch", "seq")),
        P("head"),
        P(),
        P("head", None),
    )
    out_specs = P(("batch", "seq", "head"), None)
    return jax.shard_map(body, mesh=mesh, in_specs=in_specs, out_specs=out_specs, check_vma=False)
```

```python
import functools
import jax
import jax.numpy as jnp
from jax import lax
from jax.experimental import pallas as pl
from jax.experimental.pallas import tpu as pltpu
from jax.sharding import PartitionSpec as P

HEAD_COUNT = 80
HEAD_DIM = 64
STATE = 128
GROUPS = 8
BLOCK = 256
LANES = 128
UNIT = 128
epsilon = 1e-05
HIGHEST = lax.Precision.HIGHEST
F32 = jnp.float32
BF16 = jnp.bfloat16
MESH = pl.DeviceIdType.MESH


def dot(a, b, ca, cb, precision=None):
    return lax.dot_general(
        a, b, (((ca,), (cb,)), ((), ())), precision=precision, preferred_element_type=F32
    )


def iotas(rows, columns):
    return (
        lax.broadcasted_iota(jnp.int32, (rows, columns), 0),
        lax.broadcasted_iota(jnp.int32, (rows, columns), 1),
    )


def pieces(channels, repeats):
    found = []
    for start in range(0, channels, LANES):
        width = min(LANES, channels - start)
        heads = [start // HEAD_DIM + i for i in range(width // HEAD_DIM)]
        found.append((len(found), start, width, heads, heads[0] // repeats))
    return found


def spread(columns, heads, width):
    rows = columns.shape[0]
    first = jnp.broadcast_to(columns[:, heads[0] : heads[0] + 1], (rows, width))
    if len(heads) == 1:
        return first
    second = jnp.broadcast_to(columns[:, heads[1] : heads[1] + 1], (rows, width))
    lane = iotas(rows, width)[1]
    return jnp.where(lane < HEAD_DIM, first, second)


def split(value, count):
    parts = []
    for _ in range(count):
        part = value.astype(BF16)
        parts.append(part)
        value = value - part.astype(F32)
    return parts


def column_tiles(start, stop, size):
    return [(at, min(size, stop - at)) for at in range(start, stop, size)]


def mixer_kernel(
    plan, x_hbm, gate_hbm, b_hbm, c_hbm, step_hbm, log_hbm, skip_ref, gain_ref, w_hbm, out_hbm,
    x, gate, b, c, step, log, w, stack, stack2, rows_ref, cols_ref, ends_ref, prefix, base,
    state_out, state_in, g_ref, part, squares, squares_in, first_a, first_b, second_a, second_b, stage,
    load_sem, out_sem, state_send, state_recv, square_send, square_recv,
    first_a_send, first_a_recv, first_b_send, first_b_recv,
    second_a_send, second_a_recv, second_b_send, second_b_recv,
):
    X, Y, S, groups, repeats = plan
    H = X * Y
    tokens, channels = x.shape
    model = w.shape[1]
    half = model // 2
    heads = step.shape[0]
    padded = stack.shape[0] // (tokens // BLOCK)
    blocks = tokens // BLOCK
    per_share = tokens // H
    unit = min(UNIT, per_share)
    subs = per_share // unit
    units = BLOCK // unit
    per_group = HEAD_COUNT // GROUPS
    every = pieces(channels, repeats)
    first_gain = lax.axis_index("head") * len(every) if channels % LANES == 0 else 0

    me = lax.axis_index("head")
    z = lax.axis_index("seq")
    gx = me % X
    gy = me // X
    to = lambda dx, dy: {"head": ((gy + dy) % Y) * X + (gx + dx) % X}
    after = {"seq": lax.rem(z + 1, S)}

    offset = pl.multiple_of((me * heads // per_group) // groups * (groups * STATE), STATE)
    loads = [
        pltpu.make_async_copy(log_hbm, log, load_sem.at[0]),
        pltpu.make_async_copy(step_hbm, step, load_sem.at[1]),
        pltpu.make_async_copy(b_hbm.at[:, pl.ds(offset, groups * STATE)], b, load_sem.at[2]),
        pltpu.make_async_copy(x_hbm, x, load_sem.at[3]),
        pltpu.make_async_copy(c_hbm.at[:, pl.ds(offset, groups * STATE)], c, load_sem.at[4]),
        pltpu.make_async_copy(gate_hbm, gate, load_sem.at[5]),
        pltpu.make_async_copy(w_hbm, w, load_sem.at[6]),
    ]
    for load in loads:
        load.start()

    barrier = pltpu.get_barrier_semaphore()
    for d in range(1, H):
        pl.semaphore_signal(barrier, inc=1, device_id={"head": lax.rem(me + d, H)}, device_id_type=MESH)
    if S > 1:
        @pl.when(z > 0)
        def _():
            pl.semaphore_signal(barrier, inc=1, device_id={"seq": lax.max(z - 1, 0)}, device_id_type=MESH)

        @pl.when(z < S - 1)
        def _():
            pl.semaphore_signal(barrier, inc=1, device_id=after, device_id_type=MESH)

    near = 0
    if S > 1:
        near = jnp.where(z > 0, 1, 0) + jnp.where(z < S - 1, 1, 0)
    pl.semaphore_wait(barrier, near + (H - 1))

    def state_copy(p):
        return pltpu.make_async_remote_copy(
            src_ref=state_out.at[p], dst_ref=state_in.at[p], send_sem=state_send.at[p],
            recv_sem=state_recv.at[p], device_id=after, device_id_type=MESH,
        )

    t_iota, s_iota = iotas(BLOCK, BLOCK)
    lower = jnp.where(s_iota <= t_iota, 1.0, 0.0)
    lower_b = lower.astype(BF16)
    stack[...] = jnp.zeros_like(stack)
    stack2[...] = jnp.ones_like(stack2)
    prefix[0] = jnp.zeros(prefix.shape[1:], F32)
    base[0:8] = jnp.zeros((8, channels), F32)
    state_out[...] = jnp.zeros_like(state_out)

    @pl.when(z == 0)
    def _():
        state_in[...] = jnp.zeros_like(state_in)

    loads[0].wait()
    loads[1].wait()
    for k in range(blocks):
        stack[k * padded : k * padded + heads, :] = log[:, k * BLOCK : (k + 1) * BLOCK]
        stack2[k * padded : k * padded + heads, :] = step[:, k * BLOCK : (k + 1) * BLOCK]
    rows_all, cols_all = 0.0, 0.0
    for part_of in split(stack[...], 3):
        rows_all = rows_all + dot(part_of, lower_b, 1, 1)
        cols_all = cols_all + dot(lower_b, part_of, 1, 1)
    steps = stack2[...]
    rows_ref[...] = rows_all - jnp.log(steps)
    to_end = jnp.exp(rows_all[:, BLOCK - 1 : BLOCK] - rows_all) * steps
    ends_ref[...] = to_end
    for k in range(blocks):
        cols_ref[k] = cols_all[:, k * padded : (k + 1) * padded]

    loads[2].wait()
    loads[3].wait()
    middle = (len(every) + 1) // 2
    for some in (every[:middle], every[middle:]):
        if not some:
            continue

        def state_step(k, carry, some=some):
            row = pl.ds(pl.multiple_of(k * BLOCK, BLOCK), BLOCK)
            spot = pl.ds(pl.multiple_of(k * 8, 8), 8)
            following = pl.ds(pl.multiple_of(k * 8 + 8, 8), 8)
            end = cols_ref[k, BLOCK - 8 : BLOCK, :][7:8, :]
            ends = ends_ref[pl.ds(pl.multiple_of(k * padded, padded), padded), :]
            turned = {}
            for p, start, width, of, group in some:
                lanes = slice(start, start + width)
                last = spread(end, of, width)
                if group not in turned:
                    turned[group] = b[row, group * STATE : (group + 1) * STATE].T.astype(F32)
                scaled = [(turned[group] * ends[head : head + 1, :]).astype(BF16) for head in of]
                both = dot(jnp.concatenate(scaled, axis=0), x[row, lanes], 1, 0)
                new = both[:STATE]
                if len(of) > 1:
                    new = jnp.where(iotas(STATE, width)[1] < HEAD_DIM, new, both[STATE:])
                prefix[k + 1, :, lanes] = jnp.exp(last) * prefix[k, :, lanes] + new
                base[following, lanes] = base[spot, lanes] + last
            return carry

        lax.fori_loop(0, blocks, state_step, 0)
        if S > 1:
            @pl.when(z == 0)
            def _(some=some):
                for p, start, width, of, group in some:
                    state_out[p, :, :width] = prefix[blocks, :, start : start + width].astype(BF16)
                    state_copy(p).start()

    def pass_state():
        for p, start, width, of, group in every:
            lanes = slice(start, start + width)
            state_copy(p).wait_recv()

            @pl.when(z < S - 1)
            def _():
                grown = jnp.exp(base[blocks * 8 : blocks * 8 + 1, lanes]) * state_in[p, :, :width].astype(F32)
                state_out[p, :, :width] = (grown + prefix[blocks, :, lanes]).astype(BF16)
                state_copy(p).start()

    def block_of(j):
        if per_share < BLOCK:
            return j
        chunks = per_share // BLOCK
        o = j // chunks
        dx = X - 1 - o // Y
        dy = Y - 1 - o % Y
        return (((gy + dy) % Y) * X + (gx + dx) % X) * chunks + j % chunks

    def within(j):
        k = block_of(j)
        row = pl.ds(pl.multiple_of(k * BLOCK, BLOCK), BLOCK)
        mid = BLOCK // 2
        columns = cols_ref[k]
        rows = rows_ref[pl.ds(pl.multiple_of(k * padded, padded), padded), :]
        scores = {}
        for p, start, width, of, group in every:
            lanes = slice(start, start + width)
            if group not in scores:
                which = slice(group * STATE, (group + 1) * STATE)
                scores[group] = dot(c[row, which], b[row, which], 1, 1) * lower
            x_here = x[row, lanes]
            lane = iotas(BLOCK, width)[1]
            top, bottom = 0.0, 0.0
            for i, head in enumerate(of):
                kept = (lane >= i * HEAD_DIM) & (lane < (i + 1) * HEAD_DIM)
                x_head = x_here if len(of) == 1 else jnp.where(kept, x_here, jnp.zeros_like(x_here))
                column, across = columns[:, head : head + 1], rows[head : head + 1, :]
                w_top = scores[group][:mid, :mid] * jnp.exp(
                    jnp.minimum(column[:mid] - across[:, :mid], 0.0)
                )
                w_bottom = scores[group][mid:] * jnp.exp(jnp.minimum(column[mid:] - across, 0.0))
                top = top + dot(w_top.astype(BF16), x_head[:mid], 1, 0)
                bottom = bottom + dot(w_bottom.astype(BF16), x_head, 1, 0)
            gains = jnp.full((1, width), skip_ref[of[0]], F32)
            if len(of) > 1:
                gains = jnp.where(iotas(1, width)[1] < HEAD_DIM, gains, skip_ref[of[1]])
            direct = gains * x_here.astype(F32)
            x[row, lanes] = jnp.concatenate([top + direct[:mid], bottom + direct[mid:]], axis=0).astype(BF16)

    def first_copy(buffer, send, recv, dx, dy, sub, row, columns, slot):
        return pltpu.make_async_remote_copy(
            src_ref=part.at[pl.ds(row, unit), columns],
            dst_ref=buffer.at[slot[0], slot[1], sub],
            send_sem=send.at[slot[0], slot[1], sub],
            recv_sem=recv.at[slot[0], slot[1], sub],
            device_id=to(dx, dy), device_id_type=MESH,
        )

    def copy_a(dx, dy, sub, row):
        return first_copy(
            first_a, first_a_send, first_a_recv, dx, 0, sub, row, pl.ds(0, half), (dx - 1, dy)
        )

    def copy_b(dx, dy, sub, row):
        return first_copy(
            first_b, first_b_send, first_b_recv, 0, dy, sub, row, pl.ds(half, model - half), (dy - 1, dx)
        )

    def copy_squares(dx, dy, sub, index):
        slot = dx * Y + dy
        return pltpu.make_async_remote_copy(
            src_ref=squares.at[index], dst_ref=squares_in.at[slot, sub],
            send_sem=square_send.at[slot, sub], recv_sem=square_recv.at[slot, sub],
            device_id=to(dx, dy), device_id_type=MESH,
        )

    def finish(j):
        k = block_of(j)
        row = pl.ds(pl.multiple_of(k * BLOCK, BLOCK), BLOCK)
        grow_all = jnp.exp(cols_ref[k])
        before = jnp.exp(base[pl.ds(pl.multiple_of(k * 8, 8), 8), :])
        total = {}
        for p, start, width, of, group in every:
            lanes = slice(start, start + width)
            entering = prefix[k, :, lanes] + before[0:1, lanes] * state_in[p, :, :width].astype(F32)
            moved = dot(c[row, group * STATE : (group + 1) * STATE], entering.astype(BF16), 1, 0)
            across = spread(grow_all, of, width) * moved
            v = gate[row, lanes].astype(F32)
            gated = (x[row, lanes].astype(F32) + across) * (v * (0.5 + 0.5 * jnp.tanh(0.5 * v)))
            total[width] = total.get(width, 0.0) + gated * gated
            g_ref[:, lanes] = (gated * gain_ref[pl.ds(first_gain + p, 1), :width]).astype(BF16)
        summed = jnp.zeros((8, BLOCK), F32)
        for width, value in total.items():
            for part_of in split(value, 2):
                summed = summed + dot(jnp.ones((8, width), BF16), part_of, 1, 1)
        for u in range(units):
            squares[k * units + u] = summed[:, u * unit : (u + 1) * unit]
        where = []
        for u in range(units):
            begin = pl.multiple_of(k * BLOCK + u * unit, unit)
            owner = begin // per_share
            sub = (begin % per_share) // unit
            where.append(((owner % X - gx + X) % X, (owner // X - gy + Y) % Y, sub, begin, k * units + u))
        for start, width in column_tiles(0, half, 512):
            part[row, start : start + width] = dot(g_ref[...], w[:, start : start + width], 1, 0).astype(BF16)
        for dx, dy, sub, begin, index in where:
            @pl.when(dx > 0)
            def _():
                copy_a(dx, dy, sub, begin).start()
        for start, width in column_tiles(half, model, 512):
            part[row, start : start + width] = dot(g_ref[...], w[:, start : start + width], 1, 0).astype(BF16)
        for dx, dy, sub, begin, index in where:
            @pl.when(dy > 0)
            def _():
                copy_b(dx, dy, sub, begin).start()

            @pl.when(dx + dy > 0)
            def _():
                copy_squares(dx, dy, sub, index).start()

    loads[4].wait()
    waits = jnp.where(z > 0, lax.min(z * blocks // (S - 1), blocks - 1), -1) if S > 1 else None

    def within_step(i, carry):
        within(i)
        if S > 1:
            @pl.when(i == waits)
            def _():
                pass_state()

        return carry

    def finish_step(i, carry):
        finish(i)
        return carry

    lax.fori_loop(0, blocks, within_step, 0)
    loads[5].wait()
    loads[6].wait()
    lax.fori_loop(0, blocks, finish_step, 0)

    def second_copy(buffer, send, recv, dx, dy, slot, sub, row, columns):
        return pltpu.make_async_remote_copy(
            src_ref=part.at[pl.ds(row, unit), columns], dst_ref=buffer.at[slot, sub],
            send_sem=send.at[slot, sub], recv_sem=recv.at[slot, sub],
            device_id=to(dx, dy), device_id_type=MESH,
        )

    left, right = pl.ds(0, half), pl.ds(half, model - half)

    def row_of(dx, dy, sub):
        owner = ((gy + dy) % Y) * X + (gx + dx) % X
        return pl.multiple_of(owner * per_share + sub * unit, unit)

    second_a_copy = lambda dy, sub: second_copy(
        second_a, second_a_send, second_a_recv, 0, dy, dy - 1, sub, row_of(0, dy, sub), left
    )
    second_b_copy = lambda dx, sub: second_copy(
        second_b, second_b_send, second_b_recv, dx, 0, dx - 1, sub, row_of(dx, 0, sub), right
    )

    def partial_sum(row, columns, buffer, copy, count, other, sub):
        value = part[pl.ds(row, unit), columns].astype(F32)
        for d in range(1, count):
            copy(d, other, sub, row).wait_recv()
            value = value + buffer[d - 1, other, sub].astype(F32)
        return value

    swapped_b = lambda dy, dx, sub, row: copy_b(dx, dy, sub, row)

    def relay(sub, carry):
        for dy in range(1, Y):
            row = row_of(0, dy, sub)
            part[pl.ds(row, unit), left] = partial_sum(row, left, first_a, copy_a, X, dy, sub).astype(BF16)
            second_a_copy(dy, sub).start()
        for dx in range(1, X):
            row = row_of(dx, 0, sub)
            part[pl.ds(row, unit), right] = partial_sum(row, right, first_b, swapped_b, Y, dx, sub).astype(BF16)
            second_b_copy(dx, sub).start()
        return carry

    lax.fori_loop(0, subs, relay, 0)

    def out_copy(sub):
        there = pl.ds(pl.multiple_of(sub * unit, unit), unit)
        return pltpu.make_async_copy(stage.at[there, :], out_hbm.at[there, :], out_sem.at[sub])

    same_u = jnp.where(iotas(unit, unit)[0] == iotas(unit, unit)[1], 1.0, 0.0)

    def settle(sub, carry):
        row = row_of(0, 0, sub)
        there = pl.ds(pl.multiple_of(sub * unit, unit), unit)
        summed = squares[me * subs + sub]
        for dx in range(X):
            for dy in range(Y):
                if dx + dy > 0:
                    copy_squares(dx, dy, sub, 0).wait_recv()
                    summed = summed + squares_in[dx * Y + dy, sub]
        column = dot(same_u, summed, 1, 1, HIGHEST)[:, 0:1]
        scale = lax.rsqrt(column / (HEAD_COUNT * HEAD_DIM) + epsilon)
        value = partial_sum(row, left, first_a, copy_a, X, 0, sub)
        for dy in range(1, Y):
            second_a_copy(dy, sub).wait_recv()
            value = value + second_a[dy - 1, sub].astype(F32)
        stage[there, left] = (value * scale).astype(BF16)
        value = partial_sum(row, right, first_b, swapped_b, Y, 0, sub)
        for dx in range(1, X):
            second_b_copy(dx, sub).wait_recv()
            value = value + second_b[dx - 1, sub].astype(F32)
        stage[there, right] = (value * scale).astype(BF16)
        out_copy(sub).start()
        return carry

    lax.fori_loop(0, subs, settle, 0)

    def drain(sub, carry):
        for dx in range(X):
            for dy in range(Y):
                if dx > 0:
                    copy_a(dx, dy, sub, 0).wait_send()
                if dy > 0:
                    copy_b(dx, dy, sub, 0).wait_send()
                if dx + dy > 0:
                    copy_squares(dx, dy, sub, 0).wait_send()
        for dy in range(1, Y):
            second_a_copy(dy, sub).wait_send()
        for dx in range(1, X):
            second_b_copy(dx, sub).wait_send()
        out_copy(sub).wait()
        return carry

    lax.fori_loop(0, subs, drain, 0)
    if S > 1:
        @pl.when(z < S - 1)
        def _():
            for p, start, width, of, group in every:
                state_copy(p).wait_send()


def relay_plan(homes, S, blocks, passes):
    count = len(homes)
    span, hop = 7.5, 1.5
    clock = [[0.0] * (2 * blocks + 5) for _ in range(S)]
    for z in range(S):
        now = 8.0
        for at in range(blocks):
            now = now + 1.4
            if z > 0 and at == passes[z]:
                now = max(now, 14.0 + 3.0 * z)
            clock[z][at] = now
        now = max(now, 14.0 + 3.0 * (S - 1))
        for at in range(blocks, 2 * blocks):
            now = now + 1.4
            clock[z][at] = now
        for at in range(2 * blocks, 2 * blocks + 5):
            now = now + 6.0
            clock[z][at] = now
    arrival = [[None] * count for _ in range(S)]
    taken = [{} for _ in range(S)]
    plan = [{} for _ in range(S)]
    order = [[] for _ in range(S)]
    free = {}
    for z in range(S):
        for r, m in enumerate(m for m in range(count) if homes[m] == z):
            arrival[z][m] = 2.5 + span * (r + 1)

    def send(z, m, when, step):
        begin = max(when, free.get((z, step), 0.0))
        free[z, step] = begin + span
        arrival[z + step][m] = begin + span + hop

    late = [[] for _ in range(S)]
    events = sorted((clock[z][at], z, at) for z in range(S) for at in range(2 * blocks + 5))
    for when, z, at in events:
        todo = plan[z].setdefault(at, [])
        last = at == 2 * blocks + 4
        if z == 0 or at > passes[z]:
            for m in late[z]:
                todo.append(("right", m))
                send(z, m, when, 1)
            late[z] = []
        ready = [m for m in range(count) if m not in taken[z] and arrival[z][m] is not None]
        ready = [m for m in ready if arrival[z][m] <= when + 0.2]
        for m in sorted(ready, key=lambda m: arrival[z][m]):
            taken[z][m] = at
            order[z].append(m)
            todo.append(("take", m))
            todo.append(("side", m))
            if z > 0 and homes[m] >= z:
                todo.append(("left", m))
                send(z, m, when, -1)
            if z < S - 1 and homes[m] <= z:
                if z == 0 or at > passes[z]:
                    todo.append(("right", m))
                    send(z, m, when, 1)
                else:
                    late[z].append(m)
    for z in range(S):
        rest = sorted(
            (m for m in range(count) if m not in taken[z]), key=lambda m: (abs(homes[m] - z), m)
        )
        todo = plan[z].setdefault(2 * blocks + 4, [])
        for m in rest:
            order[z].append(m)
            todo.append(("take", m))
            todo.append(("side", m))
            if z > 0 and homes[m] >= z:
                todo.append(("left", m))
            if z < S - 1 and homes[m] <= z:
                todo.append(("right", m))
    early = min(sum(1 for m in taken[z] if taken[z][m] < 2 * blocks) for z in range(S))
    return plan, order, early


def home_planes(count, S):
    sizes = [count // S] * S
    ends = [z for i in range(S) for z in ({i, S - 1 - i} if i < S - 1 - i else {i})][:S]
    for i in range(count % S):
        sizes[ends[i]] += 1
    return [z for z in range(S) for _ in range(sizes[z])]


def pair_kernel(
    plan, x_hbm, gate_hbm, b_hbm, c_hbm, step_hbm, log_hbm, skip_ref, gain_ref, w_hbm, out_hbm,
    x, gate, b, c, step, log, w, stack, stack2, rows_ref, cols_ref, ends_ref, prefix, base,
    state_out, state_in, theirs, squares, squares_in, gated_in, sums_out, sums_in, stage, scale_ref,
    load_sem, out_sem, state_send, state_recv, square_send, square_recv,
    w_send, w_recv, gated_send, gated_recv, sums_send, sums_recv,
):
    X, Y, S, groups, repeats = plan
    H = X * Y
    tokens, channels = x.shape
    model = w.shape[1]
    heads = step.shape[0]
    blocks = tokens // BLOCK
    padded = stack.shape[0] // blocks
    per_share = tokens // H
    unit = UNIT
    subs = per_share // unit
    units = BLOCK // unit
    share_blocks = per_share // BLOCK
    per_group = HEAD_COUNT // GROUPS
    every = pieces(channels, repeats)
    first_gain = lax.axis_index("head") * len(every)
    wide = 2 * LANES
    count = model // wide
    homes = home_planes(count, S)
    passes = [min(zz * blocks // (S - 1), blocks - 1) for zz in range(S)]
    tasks, order, early = relay_plan(homes, S, blocks, passes)

    me = lax.axis_index("head")
    z = lax.axis_index("seq")
    core = lax.axis_index("batch")
    gx = me % X
    gy = me // X
    to = lambda dx, dy: {"head": ((gy + dy) % Y) * X + (gx + dx) % X}
    after = {"seq": lax.rem(z + 1, S)}
    prior = {"seq": lax.max(z - 1, 0)}
    sibling = {"batch": 1 - core}

    offset = pl.multiple_of((me * heads // per_group) // groups * (groups * STATE), STATE)
    loads = [
        pltpu.make_async_copy(log_hbm, log, load_sem.at[0]),
        pltpu.make_async_copy(step_hbm, step, load_sem.at[1]),
        pltpu.make_async_copy(b_hbm.at[:, pl.ds(offset, groups * STATE)], b, load_sem.at[2]),
        pltpu.make_async_copy(x_hbm, x, load_sem.at[3]),
        pltpu.make_async_copy(c_hbm.at[:, pl.ds(offset, groups * STATE)], c, load_sem.at[4]),
        pltpu.make_async_copy(gate_hbm, gate, load_sem.at[5]),
        pltpu.make_async_copy(w_hbm, w, load_sem.at[6]),
    ]
    for load in loads:
        load.start()

    barrier = pltpu.get_barrier_semaphore()
    for d in range(1, H):
        pl.semaphore_signal(barrier, inc=1, device_id={"head": lax.rem(me + d, H)}, device_id_type=MESH)
    pl.semaphore_signal(barrier, inc=1, device_id=sibling, device_id_type=MESH)

    @pl.when(z > 0)
    def _():
        pl.semaphore_signal(barrier, inc=1, device_id=prior, device_id_type=MESH)

    @pl.when(z < S - 1)
    def _():
        pl.semaphore_signal(barrier, inc=1, device_id=after, device_id_type=MESH)

    pl.semaphore_wait(barrier, jnp.where(z > 0, 1, 0) + jnp.where(z < S - 1, 1, 0) + H)

    def held(m, which):
        return theirs.at[m, :, pl.ds(pl.multiple_of(which * LANES, LANES), LANES)]

    def w_copy(m, kind):
        source = held(m, core)
        if kind == "first":
            source = w_hbm.at[:, pl.ds(pl.multiple_of(m * wide + core * LANES, LANES), LANES)]
        return pltpu.make_async_remote_copy(
            src_ref=source, dst_ref=held(m, core),
            send_sem=w_send.at[("first", "side", "left", "right").index(kind), m],
            recv_sem=w_recv.at[m, core],
            device_id={"first": to(1, 0), "side": sibling, "left": prior, "right": after}[kind],
            device_id_type=MESH,
        )

    def w_arrival(m, which):
        return pltpu.make_async_remote_copy(
            src_ref=held(m, which), dst_ref=held(m, which), send_sem=w_send.at[0, m],
            recv_sem=w_recv.at[m, which], device_id=sibling, device_id_type=MESH,
        )

    for zz in range(S):
        @pl.when(z == zz)
        def _(zz=zz):
            for m in range(count):
                if homes[m] == zz:
                    w_copy(m, "first").start()

    def relay(at):
        for zz in range(S):
            @pl.when(z == zz)
            def _(zz=zz):
                for slot, todo in tasks[zz].items():
                    if not todo:
                        continue

                    @pl.when(at == slot)
                    def _(todo=todo):
                        for kind, m in todo:
                            if kind == "take":
                                w_arrival(m, core).wait_recv()
                            else:
                                w_copy(m, kind).start()

    def chunk_at(position):
        found = jnp.int32(0)
        for zz in range(S):
            for at in range(count):
                found = jnp.where((z == zz) & (position == at), order[zz][at], found)
        return found

    def state_copy(p):
        return pltpu.make_async_remote_copy(
            src_ref=state_out.at[p], dst_ref=state_in.at[p], send_sem=state_send.at[p],
            recv_sem=state_recv.at[p], device_id=after, device_id_type=MESH,
        )

    t_iota, s_iota = iotas(BLOCK, BLOCK)
    lower = jnp.where(s_iota <= t_iota, 1.0, 0.0)
    lower_b = lower.astype(BF16)
    stack[...] = jnp.zeros_like(stack)
    stack2[...] = jnp.ones_like(stack2)
    prefix[0] = jnp.zeros(prefix.shape[1:], F32)
    base[0:8] = jnp.zeros((8, channels), F32)
    state_out[...] = jnp.zeros_like(state_out)

    @pl.when(z == 0)
    def _():
        state_in[...] = jnp.zeros_like(state_in)

    loads[0].wait()
    loads[1].wait()
    for k in range(blocks):
        stack[k * padded : k * padded + heads, :] = log[:, k * BLOCK : (k + 1) * BLOCK]
        stack2[k * padded : k * padded + heads, :] = step[:, k * BLOCK : (k + 1) * BLOCK]
    rows_all, cols_all = 0.0, 0.0
    for part_of in split(stack[...], 3):
        rows_all = rows_all + dot(part_of, lower_b, 1, 1)
        cols_all = cols_all + dot(lower_b, part_of, 1, 1)
    steps = stack2[...]
    rows_ref[...] = rows_all - jnp.log(steps)
    to_end = jnp.exp(rows_all[:, BLOCK - 1 : BLOCK] - rows_all) * steps
    ends_ref[...] = to_end
    for k in range(blocks):
        cols_ref[k] = cols_all[:, k * padded : (k + 1) * padded]

    loads[2].wait()
    loads[3].wait()
    middle = (len(every) + 1) // 2
    for some in (every[:middle], every[middle:]):
        if not some:
            continue

        def state_step(k, carry, some=some):
            row = pl.ds(pl.multiple_of(k * BLOCK, BLOCK), BLOCK)
            spot = pl.ds(pl.multiple_of(k * 8, 8), 8)
            following = pl.ds(pl.multiple_of(k * 8 + 8, 8), 8)
            end = cols_ref[k, BLOCK - 8 : BLOCK, :][7:8, :]
            ends = ends_ref[pl.ds(pl.multiple_of(k * padded, padded), padded), :]
            turned = {}
            for p, start, width, of, group in some:
                lanes = slice(start, start + width)
                last = spread(end, of, width)
                if group not in turned:
                    turned[group] = b[row, group * STATE : (group + 1) * STATE].T.astype(F32)
                scaled = [(turned[group] * ends[head : head + 1, :]).astype(BF16) for head in of]
                both = dot(jnp.concatenate(scaled, axis=0), x[row, lanes], 1, 0)
                new = both[:STATE]
                if len(of) > 1:
                    new = jnp.where(iotas(STATE, width)[1] < HEAD_DIM, new, both[STATE:])
                prefix[k + 1, :, lanes] = jnp.exp(last) * prefix[k, :, lanes] + new
                base[following, lanes] = base[spot, lanes] + last
            return carry

        lax.fori_loop(0, blocks, state_step, 0)
        if S > 1:
            @pl.when(z == 0)
            def _(some=some):
                for p, start, width, of, group in some:
                    state_out[p, :, :width] = prefix[blocks, :, start : start + width].astype(BF16)
                    state_copy(p).start()

    def pass_state():
        for p, start, width, of, group in every:
            lanes = slice(start, start + width)
            state_copy(p).wait_recv()

            @pl.when(z < S - 1)
            def _():
                grown = jnp.exp(base[blocks * 8 : blocks * 8 + 1, lanes]) * state_in[p, :, :width].astype(F32)
                state_out[p, :, :width] = (grown + prefix[blocks, :, lanes]).astype(BF16)
                state_copy(p).start()

    def block_of(j):
        mixed = j < 2 * share_blocks
        rest = j - 2 * share_blocks
        dx = jnp.where(mixed, 1 - j % 2, 1 - rest // share_blocks)
        dy = jnp.where(mixed, 1, 0)
        sub = jnp.where(mixed, j // 2, rest % share_blocks)
        return dx, dy, sub

    def within(k):
        row = pl.ds(pl.multiple_of(k * BLOCK, BLOCK), BLOCK)
        mid = BLOCK // 2
        columns = cols_ref[k]
        rows = rows_ref[pl.ds(pl.multiple_of(k * padded, padded), padded), :]
        scores = {}
        for p, start, width, of, group in every:
            lanes = slice(start, start + width)
            if group not in scores:
                which = slice(group * STATE, (group + 1) * STATE)
                scores[group] = dot(c[row, which], b[row, which], 1, 1) * lower
            x_here = x[row, lanes]
            lane = iotas(BLOCK, width)[1]
            top, bottom = 0.0, 0.0
            for i, head in enumerate(of):
                kept = (lane >= i * HEAD_DIM) & (lane < (i + 1) * HEAD_DIM)
                x_head = x_here if len(of) == 1 else jnp.where(kept, x_here, jnp.zeros_like(x_here))
                column, across = columns[:, head : head + 1], rows[head : head + 1, :]
                w_top = scores[group][:mid, :mid] * jnp.exp(
                    jnp.minimum(column[:mid] - across[:, :mid], 0.0)
                )
                w_bottom = scores[group][mid:] * jnp.exp(jnp.minimum(column[mid:] - across, 0.0))
                top = top + dot(w_top.astype(BF16), x_head[:mid], 1, 0)
                bottom = bottom + dot(w_bottom.astype(BF16), x_head, 1, 0)
            gains = jnp.full((1, width), skip_ref[of[0]], F32)
            if len(of) > 1:
                gains = jnp.where(iotas(1, width)[1] < HEAD_DIM, gains, skip_ref[of[1]])
            direct = gains * x_here.astype(F32)
            x[row, lanes] = jnp.concatenate([top + direct[:mid], bottom + direct[mid:]], axis=0).astype(BF16)

    def row_of(dx, dy, sub):
        owner = ((gy + dy) % Y) * X + (gx + dx) % X
        return pl.multiple_of(owner * per_share + sub * unit, unit)

    def copy_gated(dy, sub):
        return pltpu.make_async_remote_copy(
            src_ref=x.at[pl.ds(row_of(1, dy, sub), unit), :], dst_ref=gated_in.at[dy, sub],
            send_sem=gated_send.at[dy, sub], recv_sem=gated_recv.at[dy, sub],
            device_id=to(1, 0), device_id_type=MESH,
        )

    def copy_squares(dx, dy, sub, index):
        slot = dx * Y + dy
        return pltpu.make_async_remote_copy(
            src_ref=squares.at[index], dst_ref=squares_in.at[slot, sub],
            send_sem=square_send.at[slot, sub], recv_sem=square_recv.at[slot, sub],
            device_id=to(dx, dy), device_id_type=MESH,
        )

    def copy_sums(sub, m):
        return pltpu.make_async_remote_copy(
            src_ref=sums_out.at[sub, m], dst_ref=sums_in.at[sub, m],
            send_sem=sums_send.at[sub, m], recv_sem=sums_recv.at[sub, m],
            device_id=to(0, 1), device_id_type=MESH,
        )

    def finish(j):
        dx, dy, part_of_share = block_of(j)
        k = row_of(dx, dy, part_of_share * units) // BLOCK
        row = pl.ds(pl.multiple_of(k * BLOCK, BLOCK), BLOCK)
        grow_all = jnp.exp(cols_ref[k])
        before = jnp.exp(base[pl.ds(pl.multiple_of(k * 8, 8), 8), :])
        total = {}
        for p, start, width, of, group in every:
            lanes = slice(start, start + width)
            entering = prefix[k, :, lanes] + before[0:1, lanes] * state_in[p, :, :width].astype(F32)
            moved = dot(c[row, group * STATE : (group + 1) * STATE], entering.astype(BF16), 1, 0)
            across = spread(grow_all, of, width) * moved
            v = gate[row, lanes].astype(F32)
            gated = (x[row, lanes].astype(F32) + across) * (v * (0.5 + 0.5 * jnp.tanh(0.5 * v)))
            total[width] = total.get(width, 0.0) + gated * gated
            x[row, lanes] = (gated * gain_ref[pl.ds(first_gain + p, 1), :width]).astype(BF16)
        summed = jnp.zeros((8, BLOCK), F32)
        for width, value in total.items():
            for part_of in split(value, 2):
                summed = summed + dot(jnp.ones((8, width), BF16), part_of, 1, 1)
        for u in range(units):
            squares[k * units + u] = summed[:, u * unit : (u + 1) * unit]

        @pl.when(dx > 0)
        def _():
            for u in range(units):
                copy_gated(dy, part_of_share * units + u).start()

        @pl.when(dx + dy > 0)
        def _():
            for u in range(units):
                copy_squares(dx, dy, part_of_share * units + u, k * units + u).start()

    def product(row, size, m, arrived):
        columns = pl.ds(pl.multiple_of(m * wide, wide), wide)
        return dot(x[pl.ds(row, size), :], w[:, columns], 1, 0) + dot(arrived, theirs[m], 1, 0)

    loads[4].wait()
    waits = jnp.where(z > 0, lax.min(z * blocks // (S - 1), blocks - 1), -1)

    def within_step(i, carry):
        within(i)

        @pl.when(i == waits)
        def _():
            pass_state()

        relay(i)
        return carry

    def finish_step(i, carry):
        finish(i)
        relay(i + blocks)
        return carry

    lax.fori_loop(0, blocks, within_step, 0)
    loads[5].wait()
    lax.fori_loop(0, blocks, finish_step, 0)
    loads[6].wait()

    def far_step(first, last, fresh, sub, carry):
        if fresh:
            copy_gated(1, sub).wait_recv()

        def tile(position, carry):
            m = chunk_at(position)

            @pl.when(sub == 0)
            def _():
                w_arrival(m, 1 - core).wait_recv()

            sums_out[sub, m] = product(row_of(0, 1, sub), unit, m, gated_in[1, sub]).astype(BF16)
            copy_sums(sub, m).start()
            return carry

        lax.fori_loop(first, last, tile, 0)
        if fresh:
            relay(2 * blocks + sub)
        return carry

    lax.fori_loop(0, subs, functools.partial(far_step, 0, early, True), 0)
    relay(2 * blocks + 4)
    lax.fori_loop(0, subs, functools.partial(far_step, early, count, False), 0)

    same_u = jnp.where(iotas(unit, unit)[0] == iotas(unit, unit)[1], 1.0, 0.0)

    def scale_step(sub, carry):
        summed = squares[me * subs + sub]
        for dx in range(X):
            for dy in range(Y):
                if dx + dy > 0:
                    copy_squares(dx, dy, sub, 0).wait_recv()
                    summed = summed + squares_in[dx * Y + dy, sub]
        column = dot(same_u, summed, 1, 1, HIGHEST)[:, 0:1]
        there = pl.ds(pl.multiple_of(sub * unit, unit), unit)
        scale_ref[there, :] = jnp.broadcast_to(lax.rsqrt(column / (HEAD_COUNT * HEAD_DIM) + epsilon), (unit, LANES))
        return carry

    lax.fori_loop(0, subs, scale_step, 0)

    def out_copy(block, m):
        there = pl.ds(pl.multiple_of(block * BLOCK, BLOCK), BLOCK)
        columns = pl.ds(pl.multiple_of(m * wide, wide), wide)
        return pltpu.make_async_copy(stage.at[there, columns], out_hbm.at[there, columns], out_sem.at[block, m])

    def near_step(first, last, fresh, block, carry):
        if fresh:
            for u in range(units):
                copy_gated(0, block * units + u).wait_recv()
        there = pl.ds(pl.multiple_of(block * BLOCK, BLOCK), BLOCK)

        def tile(position, carry):
            m = chunk_at(position)
            columns = pl.ds(pl.multiple_of(m * wide, wide), wide)
            arrived = jnp.concatenate([gated_in[0, block * units + u] for u in range(units)], axis=0)
            value = product(row_of(0, 0, block * units), BLOCK, m, arrived)
            for u in range(units):
                copy_sums(block * units + u, m).wait_recv()
            value = value + jnp.concatenate([sums_in[block * units + u, m] for u in range(units)], axis=0).astype(F32)
            scale = scale_ref[there, :]
            stage[there, columns] = (value * jnp.concatenate([scale, scale], axis=1)).astype(BF16)
            out_copy(block, m).start()
            return carry

        lax.fori_loop(first, last, tile, 0)
        return carry

    lax.fori_loop(0, share_blocks, functools.partial(near_step, 0, early, True), 0)
    lax.fori_loop(0, share_blocks, functools.partial(near_step, early, count, False), 0)

    def drain(m, carry):
        for sub in range(subs):
            copy_sums(sub, m).wait_send()
        for block in range(share_blocks):
            out_copy(block, m).wait()
        w_copy(m, "side").wait_send()
        return carry

    lax.fori_loop(0, count, drain, 0)
    for sub in range(subs):
        for dy in range(Y):
            copy_gated(dy, sub).wait_send()
        for dx in range(X):
            for dy in range(Y):
                if dx + dy > 0:
                    copy_squares(dx, dy, sub, 0).wait_send()
    for zz in range(S):
        @pl.when(z == zz)
        def _(zz=zz):
            for m in range(count):
                if homes[m] == zz:
                    w_copy(m, "first").wait_send()
                if zz > 0 and homes[m] >= zz:
                    w_copy(m, "left").wait_send()
                if zz < S - 1 and homes[m] <= zz:
                    w_copy(m, "right").wait_send()

    @pl.when(z < S - 1)
    def _():
        for p, start, width, of, group in every:
            state_copy(p).wait_send()


def body(
    ssm_input, gate_input, b_proj, c_proj, step_size, log_decay, skip_gain, norm_gain, out_weight
):
    tokens, channels = ssm_input.shape
    heads = step_size.shape[0]
    blocks = tokens // BLOCK
    model = out_weight.shape[1]
    half = model // 2
    per_group = HEAD_COUNT // GROUPS
    groups = max(1, heads // per_group)
    repeats = min(heads, per_group)
    H = lax.axis_size("head")
    S = lax.axis_size("seq")
    X = max(d for d in range(1, H + 1) if H % d == 0 and d * d <= H)
    Y = H // X
    per_share = tokens // H
    unit = min(UNIT, per_share)
    subs = per_share // unit
    count = len(pieces(channels, repeats))
    padded = -(-heads // 8) * 8
    head_index = lax.axis_index("head")
    gain = norm_gain
    if channels % LANES != 0:
        gain = lax.dynamic_slice_in_dim(norm_gain, head_index * channels, channels)
        gain = jnp.pad(gain, (0, count * LANES - channels))
    gain = gain.reshape(-1, LANES)
    anywhere = pl.BlockSpec(memory_space=pl.ANY)
    vmem = pl.BlockSpec(memory_space=pltpu.VMEM)
    dma = pltpu.SemaphoreType.DMA
    x1, y1 = max(X - 1, 1), max(Y - 1, 1)
    side = [anywhere] * 6 + [pl.BlockSpec(memory_space=pltpu.SMEM), vmem, anywhere]
    paired = (
        X == 2 and Y == 2 and S > 1 and lax.axis_size("batch") == 2 and per_share % BLOCK == 0
        and model % (2 * LANES) == 0 and channels % LANES == 0 and model // (2 * LANES) >= S
        and per_share == 4 * UNIT
    )
    common = [
        pltpu.VMEM((tokens, channels), BF16),
        pltpu.VMEM((tokens, channels), BF16),
        pltpu.VMEM((tokens, groups * STATE), BF16),
        pltpu.VMEM((tokens, groups * STATE), BF16),
        pltpu.VMEM((heads, tokens), F32),
        pltpu.VMEM((heads, tokens), F32),
        pltpu.VMEM((channels, model), BF16),
        pltpu.VMEM((blocks * padded, BLOCK), F32),
        pltpu.VMEM((blocks * padded, BLOCK), F32),
        pltpu.VMEM((blocks * padded, BLOCK), F32),
        pltpu.VMEM((blocks, BLOCK, padded), F32),
        pltpu.VMEM((blocks * padded, BLOCK), F32),
        pltpu.VMEM((blocks + 1, STATE, channels), F32),
        pltpu.VMEM(((blocks + 1) * 8, channels), F32),
        pltpu.VMEM((count, STATE, LANES), BF16),
        pltpu.VMEM((count, STATE, LANES), BF16),
    ]
    cost = pl.CostEstimate(
        flops=2 * tokens * channels * (model + 4 * BLOCK), bytes_accessed=tokens * channels * 8, transcendentals=0
    )
    params = pltpu.CompilerParams(
        collective_id=0, has_side_effects=True, vmem_limit_bytes=62 * 1024 * 1024
    )
    if paired:
        tiles = model // (2 * LANES)
        return pl.pallas_call(
            functools.partial(pair_kernel, (X, Y, S, groups, repeats)),
            in_specs=side,
            out_specs=anywhere,
            out_shape=jax.ShapeDtypeStruct((per_share, model), BF16),
            scratch_shapes=common + [
                pltpu.VMEM((tiles, channels, 2 * LANES), BF16),
                pltpu.VMEM((tokens // unit, 8, unit), F32),
                pltpu.VMEM((H, subs, 8, unit), F32),
                pltpu.VMEM((Y, subs, unit, channels), BF16),
                pltpu.VMEM((subs, tiles, unit, 2 * LANES), BF16),
                pltpu.VMEM((subs, tiles, unit, 2 * LANES), BF16),
                pltpu.VMEM((per_share, model), BF16),
                pltpu.VMEM((per_share, LANES), F32),
                dma((7,)),
                dma((per_share // BLOCK, tiles)),
                dma((count,)),
                dma((count,)),
                dma((H, subs)),
                dma((H, subs)),
                dma((4, tiles)),
                dma((tiles, 2)),
                dma((Y, subs)),
                dma((Y, subs)),
                dma((subs, tiles)),
                dma((subs, tiles)),
            ],
            compiler_params=params,
            name="mixer_pair",
            cost_estimate=cost,
        )(ssm_input, gate_input, b_proj, c_proj, step_size, log_decay, skip_gain, gain, out_weight)
    return pl.pallas_call(
        functools.partial(mixer_kernel, (X, Y, S, groups, repeats)),
        in_specs=side,
        out_specs=anywhere,
        out_shape=jax.ShapeDtypeStruct((per_share, model), BF16),
        scratch_shapes=common + [
            pltpu.VMEM((BLOCK, channels), BF16),
            pltpu.VMEM((tokens, model), BF16),
            pltpu.VMEM((tokens // unit, 8, unit), F32),
            pltpu.VMEM((H, subs, 8, unit), F32),
            pltpu.VMEM((x1, Y, subs, unit, half), BF16),
            pltpu.VMEM((y1, X, subs, unit, model - half), BF16),
            pltpu.VMEM((y1, subs, unit, half), BF16),
            pltpu.VMEM((x1, subs, unit, model - half), BF16),
            pltpu.VMEM((per_share, model), BF16),
            dma((7,)),
            dma((subs,)),
            dma((count,)),
            dma((count,)),
            dma((H, subs)),
            dma((H, subs)),
            dma((x1, Y, subs)),
            dma((x1, Y, subs)),
            dma((y1, X, subs)),
            dma((y1, X, subs)),
            dma((y1, subs)),
            dma((y1, subs)),
            dma((x1, subs)),
            dma((x1, subs)),
        ],
        compiler_params=params,
        name="mixer",
        cost_estimate=cost,
    )(ssm_input, gate_input, b_proj, c_proj, step_size, log_decay, skip_gain, gain, out_weight)


def solution(mesh):
    in_specs = (
        P(("batch", "seq"), "head"),
        P(("batch", "seq"), "head"),
        P(("batch", "seq"), None),
        P(("batch", "seq"), None),
        P("head", ("batch", "seq")),
        P("head", ("batch", "seq")),
        P("head"),
        P(),
        P("head", None),
    )
    out_specs = P(("batch", "seq", "head"), None)
    return jax.shard_map(body, mesh=mesh, in_specs=in_specs, out_specs=out_specs, check_vma=False)
```

```python
import functools
import jax
import jax.numpy as jnp
from jax import lax
from jax.experimental import pallas as pl
from jax.experimental.pallas import tpu as pltpu
from jax.sharding import PartitionSpec as P

HEAD_COUNT = 80
HEAD_DIM = 64
STATE = 128
GROUPS = 8
BLOCK = 256
LANES = 128
UNIT = 128
epsilon = 1e-05
HIGHEST = lax.Precision.HIGHEST
F32 = jnp.float32
BF16 = jnp.bfloat16
MESH = pl.DeviceIdType.MESH


def dot(a, b, ca, cb, precision=None):
    return lax.dot_general(
        a, b, (((ca,), (cb,)), ((), ())), precision=precision, preferred_element_type=F32
    )


def iotas(rows, columns):
    return (
        lax.broadcasted_iota(jnp.int32, (rows, columns), 0),
        lax.broadcasted_iota(jnp.int32, (rows, columns), 1),
    )


def pieces(channels, repeats):
    found = []
    for start in range(0, channels, LANES):
        width = min(LANES, channels - start)
        heads = [start // HEAD_DIM + i for i in range(width // HEAD_DIM)]
        found.append((len(found), start, width, heads, heads[0] // repeats))
    return found


def spread(columns, heads, width):
    rows = columns.shape[0]
    first = jnp.broadcast_to(columns[:, heads[0] : heads[0] + 1], (rows, width))
    if len(heads) == 1:
        return first
    second = jnp.broadcast_to(columns[:, heads[1] : heads[1] + 1], (rows, width))
    lane = iotas(rows, width)[1]
    return jnp.where(lane < HEAD_DIM, first, second)


def split(value, count):
    parts = []
    for _ in range(count):
        part = value.astype(BF16)
        parts.append(part)
        value = value - part.astype(F32)
    return parts


def column_tiles(start, stop, size):
    return [(at, min(size, stop - at)) for at in range(start, stop, size)]


def mixer_kernel(
    plan, x_hbm, gate_hbm, b_hbm, c_hbm, step_hbm, log_hbm, skip_ref, gain_ref, w_hbm, out_hbm,
    x, gate, b, c, step, log, w, stack, stack2, rows_ref, cols_ref, ends_ref, prefix, base,
    state_out, state_in, g_ref, part, squares, squares_in, first_a, first_b, second_a, second_b, stage,
    load_sem, out_sem, state_send, state_recv, square_send, square_recv,
    first_a_send, first_a_recv, first_b_send, first_b_recv,
    second_a_send, second_a_recv, second_b_send, second_b_recv,
):
    X, Y, S, groups, repeats = plan
    H = X * Y
    tokens, channels = x.shape
    model = w.shape[1]
    half = model // 2
    heads = step.shape[0]
    padded = stack.shape[0] // (tokens // BLOCK)
    blocks = tokens // BLOCK
    per_share = tokens // H
    unit = min(UNIT, per_share)
    subs = per_share // unit
    units = BLOCK // unit
    per_group = HEAD_COUNT // GROUPS
    every = pieces(channels, repeats)
    first_gain = lax.axis_index("head") * len(every) if channels % LANES == 0 else 0

    me = lax.axis_index("head")
    z = lax.axis_index("seq")
    gx = me % X
    gy = me // X
    to = lambda dx, dy: {"head": ((gy + dy) % Y) * X + (gx + dx) % X}
    after = {"seq": lax.rem(z + 1, S)}

    offset = pl.multiple_of((me * heads // per_group) // groups * (groups * STATE), STATE)
    loads = [
        pltpu.make_async_copy(log_hbm, log, load_sem.at[0]),
        pltpu.make_async_copy(step_hbm, step, load_sem.at[1]),
        pltpu.make_async_copy(b_hbm.at[:, pl.ds(offset, groups * STATE)], b, load_sem.at[2]),
        pltpu.make_async_copy(x_hbm, x, load_sem.at[3]),
        pltpu.make_async_copy(c_hbm.at[:, pl.ds(offset, groups * STATE)], c, load_sem.at[4]),
        pltpu.make_async_copy(gate_hbm, gate, load_sem.at[5]),
        pltpu.make_async_copy(w_hbm, w, load_sem.at[6]),
    ]
    for load in loads:
        load.start()

    barrier = pltpu.get_barrier_semaphore()
    for d in range(1, H):
        pl.semaphore_signal(barrier, inc=1, device_id={"head": lax.rem(me + d, H)}, device_id_type=MESH)
    if S > 1:
        @pl.when(z > 0)
        def _():
            pl.semaphore_signal(barrier, inc=1, device_id={"seq": lax.max(z - 1, 0)}, device_id_type=MESH)

        @pl.when(z < S - 1)
        def _():
            pl.semaphore_signal(barrier, inc=1, device_id=after, device_id_type=MESH)

    near = 0
    if S > 1:
        near = jnp.where(z > 0, 1, 0) + jnp.where(z < S - 1, 1, 0)
    pl.semaphore_wait(barrier, near + (H - 1))

    def state_copy(p):
        return pltpu.make_async_remote_copy(
            src_ref=state_out.at[p], dst_ref=state_in.at[p], send_sem=state_send.at[p],
            recv_sem=state_recv.at[p], device_id=after, device_id_type=MESH,
        )

    t_iota, s_iota = iotas(BLOCK, BLOCK)
    lower = jnp.where(s_iota <= t_iota, 1.0, 0.0)
    lower_b = lower.astype(BF16)
    stack[...] = jnp.zeros_like(stack)
    stack2[...] = jnp.ones_like(stack2)
    prefix[0] = jnp.zeros(prefix.shape[1:], F32)
    base[0:8] = jnp.zeros((8, channels), F32)
    state_out[...] = jnp.zeros_like(state_out)

    @pl.when(z == 0)
    def _():
        state_in[...] = jnp.zeros_like(state_in)

    loads[0].wait()
    loads[1].wait()
    for k in range(blocks):
        stack[k * padded : k * padded + heads, :] = log[:, k * BLOCK : (k + 1) * BLOCK]
        stack2[k * padded : k * padded + heads, :] = step[:, k * BLOCK : (k + 1) * BLOCK]
    rows_all, cols_all = 0.0, 0.0
    for part_of in split(stack[...], 3):
        rows_all = rows_all + dot(part_of, lower_b, 1, 1)
        cols_all = cols_all + dot(lower_b, part_of, 1, 1)
    steps = stack2[...]
    rows_ref[...] = rows_all - jnp.log(steps)
    to_end = jnp.exp(rows_all[:, BLOCK - 1 : BLOCK] - rows_all) * steps
    ends_ref[...] = to_end
    for k in range(blocks):
        cols_ref[k] = cols_all[:, k * padded : (k + 1) * padded]

    loads[2].wait()
    loads[3].wait()
    middle = (len(every) + 1) // 2
    for some in (every[:middle], every[middle:]):
        if not some:
            continue

        def state_step(k, carry, some=some):
            row = pl.ds(pl.multiple_of(k * BLOCK, BLOCK), BLOCK)
            spot = pl.ds(pl.multiple_of(k * 8, 8), 8)
            following = pl.ds(pl.multiple_of(k * 8 + 8, 8), 8)
            end = cols_ref[k, BLOCK - 8 : BLOCK, :][7:8, :]
            ends = ends_ref[pl.ds(pl.multiple_of(k * padded, padded), padded), :]
            turned = {}
            for p, start, width, of, group in some:
                lanes = slice(start, start + width)
                last = spread(end, of, width)
                if group not in turned:
                    turned[group] = b[row, group * STATE : (group + 1) * STATE].T.astype(F32)
                scaled = [(turned[group] * ends[head : head + 1, :]).astype(BF16) for head in of]
                both = dot(jnp.concatenate(scaled, axis=0), x[row, lanes], 1, 0)
                new = both[:STATE]
                if len(of) > 1:
                    new = jnp.where(iotas(STATE, width)[1] < HEAD_DIM, new, both[STATE:])
                prefix[k + 1, :, lanes] = jnp.exp(last) * prefix[k, :, lanes] + new
                base[following, lanes] = base[spot, lanes] + last
            return carry

        lax.fori_loop(0, blocks, state_step, 0)
        if S > 1:
            @pl.when(z == 0)
            def _(some=some):
                for p, start, width, of, group in some:
                    state_out[p, :, :width] = prefix[blocks, :, start : start + width].astype(BF16)
                    state_copy(p).start()

    def pass_state():
        for p, start, width, of, group in every:
            lanes = slice(start, start + width)
            state_copy(p).wait_recv()

            @pl.when(z < S - 1)
            def _():
                grown = jnp.exp(base[blocks * 8 : blocks * 8 + 1, lanes]) * state_in[p, :, :width].astype(F32)
                state_out[p, :, :width] = (grown + prefix[blocks, :, lanes]).astype(BF16)
                state_copy(p).start()

    def block_of(j):
        if per_share < BLOCK:
            return j
        chunks = per_share // BLOCK
        o = j // chunks
        dx = X - 1 - o // Y
        dy = Y - 1 - o % Y
        return (((gy + dy) % Y) * X + (gx + dx) % X) * chunks + j % chunks

    def within(j):
        k = block_of(j)
        row = pl.ds(pl.multiple_of(k * BLOCK, BLOCK), BLOCK)
        mid = BLOCK // 2
        columns = cols_ref[k]
        rows = rows_ref[pl.ds(pl.multiple_of(k * padded, padded), padded), :]
        scores = {}
        for p, start, width, of, group in every:
            lanes = slice(start, start + width)
            if group not in scores:
                which = slice(group * STATE, (group + 1) * STATE)
                scores[group] = dot(c[row, which], b[row, which], 1, 1) * lower
            x_here = x[row, lanes]
            lane = iotas(BLOCK, width)[1]
            top, bottom = 0.0, 0.0
            for i, head in enumerate(of):
                kept = (lane >= i * HEAD_DIM) & (lane < (i + 1) * HEAD_DIM)
                x_head = x_here if len(of) == 1 else jnp.where(kept, x_here, jnp.zeros_like(x_here))
                column, across = columns[:, head : head + 1], rows[head : head + 1, :]
                w_top = scores[group][:mid, :mid] * jnp.exp(
                    jnp.minimum(column[:mid] - across[:, :mid], 0.0)
                )
                w_bottom = scores[group][mid:] * jnp.exp(jnp.minimum(column[mid:] - across, 0.0))
                top = top + dot(w_top.astype(BF16), x_head[:mid], 1, 0)
                bottom = bottom + dot(w_bottom.astype(BF16), x_head, 1, 0)
            gains = jnp.full((1, width), skip_ref[of[0]], F32)
            if len(of) > 1:
                gains = jnp.where(iotas(1, width)[1] < HEAD_DIM, gains, skip_ref[of[1]])
            direct = gains * x_here.astype(F32)
            x[row, lanes] = jnp.concatenate([top + direct[:mid], bottom + direct[mid:]], axis=0).astype(BF16)

    def first_copy(buffer, send, recv, dx, dy, sub, row, columns, slot):
        return pltpu.make_async_remote_copy(
            src_ref=part.at[pl.ds(row, unit), columns],
            dst_ref=buffer.at[slot[0], slot[1], sub],
            send_sem=send.at[slot[0], slot[1], sub],
            recv_sem=recv.at[slot[0], slot[1], sub],
            device_id=to(dx, dy), device_id_type=MESH,
        )

    def copy_a(dx, dy, sub, row):
        return first_copy(
            first_a, first_a_send, first_a_recv, dx, 0, sub, row, pl.ds(0, half), (dx - 1, dy)
        )

    def copy_b(dx, dy, sub, row):
        return first_copy(
            first_b, first_b_send, first_b_recv, 0, dy, sub, row, pl.ds(half, model - half), (dy - 1, dx)
        )

    def copy_squares(dx, dy, sub, index):
        slot = dx * Y + dy
        return pltpu.make_async_remote_copy(
            src_ref=squares.at[index], dst_ref=squares_in.at[slot, sub],
            send_sem=square_send.at[slot, sub], recv_sem=square_recv.at[slot, sub],
            device_id=to(dx, dy), device_id_type=MESH,
        )

    def finish(j):
        k = block_of(j)
        row = pl.ds(pl.multiple_of(k * BLOCK, BLOCK), BLOCK)
        grow_all = jnp.exp(cols_ref[k])
        before = jnp.exp(base[pl.ds(pl.multiple_of(k * 8, 8), 8), :])
        total = {}
        for p, start, width, of, group in every:
            lanes = slice(start, start + width)
            entering = prefix[k, :, lanes] + before[0:1, lanes] * state_in[p, :, :width].astype(F32)
            moved = dot(c[row, group * STATE : (group + 1) * STATE], entering.astype(BF16), 1, 0)
            across = spread(grow_all, of, width) * moved
            v = gate[row, lanes].astype(F32)
            gated = (x[row, lanes].astype(F32) + across) * (v * (0.5 + 0.5 * jnp.tanh(0.5 * v)))
            total[width] = total.get(width, 0.0) + gated * gated
            g_ref[:, lanes] = (gated * gain_ref[pl.ds(first_gain + p, 1), :width]).astype(BF16)
        summed = jnp.zeros((8, BLOCK), F32)
        for width, value in total.items():
            for part_of in split(value, 2):
                summed = summed + dot(jnp.ones((8, width), BF16), part_of, 1, 1)
        for u in range(units):
            squares[k * units + u] = summed[:, u * unit : (u + 1) * unit]
        where = []
        for u in range(units):
            begin = pl.multiple_of(k * BLOCK + u * unit, unit)
            owner = begin // per_share
            sub = (begin % per_share) // unit
            where.append(((owner % X - gx + X) % X, (owner // X - gy + Y) % Y, sub, begin, k * units + u))
        for start, width in column_tiles(0, half, 512):
            part[row, start : start + width] = dot(g_ref[...], w[:, start : start + width], 1, 0).astype(BF16)
        for dx, dy, sub, begin, index in where:
            @pl.when(dx > 0)
            def _():
                copy_a(dx, dy, sub, begin).start()
        for start, width in column_tiles(half, model, 512):
            part[row, start : start + width] = dot(g_ref[...], w[:, start : start + width], 1, 0).astype(BF16)
        for dx, dy, sub, begin, index in where:
            @pl.when(dy > 0)
            def _():
                copy_b(dx, dy, sub, begin).start()

            @pl.when(dx + dy > 0)
            def _():
                copy_squares(dx, dy, sub, index).start()

    loads[4].wait()
    waits = jnp.where(z > 0, lax.min(z * blocks // (S - 1), blocks - 1), -1) if S > 1 else None

    def within_step(i, carry):
        within(i)
        if S > 1:
            @pl.when(i == waits)
            def _():
                pass_state()

        return carry

    def finish_step(i, carry):
        finish(i)
        return carry

    lax.fori_loop(0, blocks, within_step, 0)
    loads[5].wait()
    loads[6].wait()
    lax.fori_loop(0, blocks, finish_step, 0)

    def second_copy(buffer, send, recv, dx, dy, slot, sub, row, columns):
        return pltpu.make_async_remote_copy(
            src_ref=part.at[pl.ds(row, unit), columns], dst_ref=buffer.at[slot, sub],
            send_sem=send.at[slot, sub], recv_sem=recv.at[slot, sub],
            device_id=to(dx, dy), device_id_type=MESH,
        )

    left, right = pl.ds(0, half), pl.ds(half, model - half)

    def row_of(dx, dy, sub):
        owner = ((gy + dy) % Y) * X + (gx + dx) % X
        return pl.multiple_of(owner * per_share + sub * unit, unit)

    second_a_copy = lambda dy, sub: second_copy(
        second_a, second_a_send, second_a_recv, 0, dy, dy - 1, sub, row_of(0, dy, sub), left
    )
    second_b_copy = lambda dx, sub: second_copy(
        second_b, second_b_send, second_b_recv, dx, 0, dx - 1, sub, row_of(dx, 0, sub), right
    )

    def partial_sum(row, columns, buffer, copy, count, other, sub):
        value = part[pl.ds(row, unit), columns].astype(F32)
        for d in range(1, count):
            copy(d, other, sub, row).wait_recv()
            value = value + buffer[d - 1, other, sub].astype(F32)
        return value

    swapped_b = lambda dy, dx, sub, row: copy_b(dx, dy, sub, row)

    def relay(sub, carry):
        for dy in range(1, Y):
            row = row_of(0, dy, sub)
            part[pl.ds(row, unit), left] = partial_sum(row, left, first_a, copy_a, X, dy, sub).astype(BF16)
            second_a_copy(dy, sub).start()
        for dx in range(1, X):
            row = row_of(dx, 0, sub)
            part[pl.ds(row, unit), right] = partial_sum(row, right, first_b, swapped_b, Y, dx, sub).astype(BF16)
            second_b_copy(dx, sub).start()
        return carry

    lax.fori_loop(0, subs, relay, 0)

    def out_copy(sub):
        there = pl.ds(pl.multiple_of(sub * unit, unit), unit)
        return pltpu.make_async_copy(stage.at[there, :], out_hbm.at[there, :], out_sem.at[sub])

    same_u = jnp.where(iotas(unit, unit)[0] == iotas(unit, unit)[1], 1.0, 0.0)

    def settle(sub, carry):
        row = row_of(0, 0, sub)
        there = pl.ds(pl.multiple_of(sub * unit, unit), unit)
        summed = squares[me * subs + sub]
        for dx in range(X):
            for dy in range(Y):
                if dx + dy > 0:
                    copy_squares(dx, dy, sub, 0).wait_recv()
                    summed = summed + squares_in[dx * Y + dy, sub]
        column = dot(same_u, summed, 1, 1, HIGHEST)[:, 0:1]
        scale = lax.rsqrt(column / (HEAD_COUNT * HEAD_DIM) + epsilon)
        value = partial_sum(row, left, first_a, copy_a, X, 0, sub)
        for dy in range(1, Y):
            second_a_copy(dy, sub).wait_recv()
            value = value + second_a[dy - 1, sub].astype(F32)
        stage[there, left] = (value * scale).astype(BF16)
        value = partial_sum(row, right, first_b, swapped_b, Y, 0, sub)
        for dx in range(1, X):
            second_b_copy(dx, sub).wait_recv()
            value = value + second_b[dx - 1, sub].astype(F32)
        stage[there, right] = (value * scale).astype(BF16)
        out_copy(sub).start()
        return carry

    lax.fori_loop(0, subs, settle, 0)

    def drain(sub, carry):
        for dx in range(X):
            for dy in range(Y):
                if dx > 0:
                    copy_a(dx, dy, sub, 0).wait_send()
                if dy > 0:
                    copy_b(dx, dy, sub, 0).wait_send()
                if dx + dy > 0:
                    copy_squares(dx, dy, sub, 0).wait_send()
        for dy in range(1, Y):
            second_a_copy(dy, sub).wait_send()
        for dx in range(1, X):
            second_b_copy(dx, sub).wait_send()
        out_copy(sub).wait()
        return carry

    lax.fori_loop(0, subs, drain, 0)
    if S > 1:
        @pl.when(z < S - 1)
        def _():
            for p, start, width, of, group in every:
                state_copy(p).wait_send()


def relay_plan(homes, S, blocks, passes):
    count = len(homes)
    span, hop = 7.5, 1.5
    clock = [[0.0] * (2 * blocks + 4) for _ in range(S)]
    for z in range(S):
        now = 8.0
        for at in range(blocks):
            now = now + 1.4
            if z > 0 and at == passes[z]:
                now = max(now, 14.0 + 3.0 * z)
            clock[z][at] = now
        now = max(now, 14.0 + 3.0 * (S - 1))
        for at in range(blocks, 2 * blocks):
            now = now + 1.4
            clock[z][at] = now
        for at in range(2 * blocks, 2 * blocks + 4):
            now = now + 7.5
            clock[z][at] = now
    arrival = [[None] * count for _ in range(S)]
    taken = [{} for _ in range(S)]
    plan = [{} for _ in range(S)]
    order = [[] for _ in range(S)]
    free = {}
    for z in range(S):
        for r, m in enumerate(m for m in range(count) if homes[m] == z):
            arrival[z][m] = 2.5 + span * (r + 1)

    def send(z, m, when, step):
        begin = max(when, free.get((z, step), 0.0))
        free[z, step] = begin + span
        arrival[z + step][m] = begin + span + hop

    late = [[] for _ in range(S)]
    events = sorted((clock[z][at], z, at) for z in range(S) for at in range(2 * blocks + 4))
    for when, z, at in events:
        todo = plan[z].setdefault(at, [])
        if z == 0 or at > passes[z]:
            for m in late[z]:
                todo.append(("right", m))
                send(z, m, when, 1)
            late[z] = []
        ready = [m for m in range(count) if m not in taken[z] and arrival[z][m] is not None]
        ready = [m for m in ready if arrival[z][m] <= when + 0.2]
        for m in sorted(ready, key=lambda m: arrival[z][m]):
            taken[z][m] = at
            order[z].append(m)
            todo.append(("take", m))
            todo.append(("side", m))
            if z > 0 and homes[m] >= z:
                todo.append(("left", m))
                send(z, m, when, -1)
            if z < S - 1 and homes[m] <= z:
                if z == 0 or at > passes[z]:
                    todo.append(("right", m))
                    send(z, m, when, 1)
                else:
                    late[z].append(m)
    final = [{} for _ in range(S)]
    for z in range(S):
        rest = [m for m in range(count) if m not in taken[z]]
        for m in sorted(rest, key=lambda m: (abs(homes[m] - z), m)):
            todo = final[z].setdefault(len(order[z]), [("take", m), ("side", m)])
            order[z].append(m)
            if z > 0 and homes[m] >= z:
                todo.append(("left", m))
            if z < S - 1 and homes[m] <= z:
                todo.append(("right", m))
    ready = [
        min(sum(1 for m in taken[z] if taken[z][m] < at) for z in range(S))
        for at in range(2 * blocks, 2 * blocks + 5)
    ]
    return plan, final, order, ready


def home_planes(count, S):
    sizes = [count // S] * S
    ends = [z for i in range(S) for z in ({i, S - 1 - i} if i < S - 1 - i else {i})][:S]
    for i in range(count % S):
        sizes[ends[i]] += 1
    return [z for z in range(S) for _ in range(sizes[z])]


def pair_kernel(
    plan, x_hbm, gate_hbm, b_hbm, c_hbm, step_hbm, log_hbm, skip_ref, gain_ref, w_hbm, out_hbm,
    x, gate, b, c, step, log, w, stack, stack2, rows_ref, cols_ref, ends_ref, prefix, base,
    state_out, state_in, theirs, squares, squares_in, gated_in, sums_out, sums_in, stage, scale_ref,
    load_sem, out_sem, state_send, state_recv, square_send, square_recv,
    w_send, w_recv, gated_send, gated_recv, sums_send, sums_recv,
):
    X, Y, S, groups, repeats = plan
    H = X * Y
    tokens, channels = x.shape
    model = w.shape[1]
    heads = step.shape[0]
    blocks = tokens // BLOCK
    padded = stack.shape[0] // blocks
    per_share = tokens // H
    unit = UNIT
    subs = per_share // unit
    units = BLOCK // unit
    share_blocks = per_share // BLOCK
    per_group = HEAD_COUNT // GROUPS
    every = pieces(channels, repeats)
    first_gain = lax.axis_index("head") * len(every)
    wide = 2 * LANES
    count = model // wide
    homes = home_planes(count, S)
    passes = [min(zz * blocks // (S - 1), blocks - 1) for zz in range(S)]
    tasks, final, order, ready = relay_plan(homes, S, blocks, passes)

    me = lax.axis_index("head")
    z = lax.axis_index("seq")
    core = lax.axis_index("batch")
    gx = me % X
    gy = me // X
    to = lambda dx, dy: {"head": ((gy + dy) % Y) * X + (gx + dx) % X}
    after = {"seq": lax.rem(z + 1, S)}
    prior = {"seq": lax.max(z - 1, 0)}
    sibling = {"batch": 1 - core}

    offset = pl.multiple_of((me * heads // per_group) // groups * (groups * STATE), STATE)
    loads = [
        pltpu.make_async_copy(log_hbm, log, load_sem.at[0]),
        pltpu.make_async_copy(step_hbm, step, load_sem.at[1]),
        pltpu.make_async_copy(b_hbm.at[:, pl.ds(offset, groups * STATE)], b, load_sem.at[2]),
        pltpu.make_async_copy(x_hbm, x, load_sem.at[3]),
        pltpu.make_async_copy(c_hbm.at[:, pl.ds(offset, groups * STATE)], c, load_sem.at[4]),
        pltpu.make_async_copy(gate_hbm, gate, load_sem.at[5]),
        pltpu.make_async_copy(w_hbm, w, load_sem.at[6]),
    ]
    for load in loads:
        load.start()

    barrier = pltpu.get_barrier_semaphore()
    for d in range(1, H):
        pl.semaphore_signal(barrier, inc=1, device_id={"head": lax.rem(me + d, H)}, device_id_type=MESH)
    pl.semaphore_signal(barrier, inc=1, device_id=sibling, device_id_type=MESH)

    @pl.when(z > 0)
    def _():
        pl.semaphore_signal(barrier, inc=1, device_id=prior, device_id_type=MESH)

    @pl.when(z < S - 1)
    def _():
        pl.semaphore_signal(barrier, inc=1, device_id=after, device_id_type=MESH)

    pl.semaphore_wait(barrier, jnp.where(z > 0, 1, 0) + jnp.where(z < S - 1, 1, 0) + H)

    def held(m, which):
        return theirs.at[m, :, pl.ds(pl.multiple_of(which * LANES, LANES), LANES)]

    def w_copy(m, kind):
        source = held(m, core)
        if kind == "first":
            source = w_hbm.at[:, pl.ds(pl.multiple_of(m * wide + core * LANES, LANES), LANES)]
        return pltpu.make_async_remote_copy(
            src_ref=source, dst_ref=held(m, core),
            send_sem=w_send.at[("first", "side", "left", "right").index(kind), m],
            recv_sem=w_recv.at[m, core],
            device_id={"first": to(1, 0), "side": sibling, "left": prior, "right": after}[kind],
            device_id_type=MESH,
        )

    def w_arrival(m, which):
        return pltpu.make_async_remote_copy(
            src_ref=held(m, which), dst_ref=held(m, which), send_sem=w_send.at[0, m],
            recv_sem=w_recv.at[m, which], device_id=sibling, device_id_type=MESH,
        )

    for zz in range(S):
        @pl.when(z == zz)
        def _(zz=zz):
            for m in range(count):
                if homes[m] == zz:
                    w_copy(m, "first").start()

    def relay(at, tasks=tasks):
        for zz in range(S):
            @pl.when(z == zz)
            def _(zz=zz):
                for slot, todo in tasks[zz].items():
                    if not todo:
                        continue

                    @pl.when(at == slot)
                    def _(todo=todo):
                        for kind, m in todo:
                            if kind == "take":
                                w_arrival(m, core).wait_recv()
                            else:
                                w_copy(m, kind).start()

    def chunk_at(position):
        found = jnp.int32(0)
        for zz in range(S):
            for at in range(count):
                found = jnp.where((z == zz) & (position == at), order[zz][at], found)
        return found

    def state_copy(p):
        return pltpu.make_async_remote_copy(
            src_ref=state_out.at[p], dst_ref=state_in.at[p], send_sem=state_send.at[p],
            recv_sem=state_recv.at[p], device_id=after, device_id_type=MESH,
        )

    t_iota, s_iota = iotas(BLOCK, BLOCK)
    lower = jnp.where(s_iota <= t_iota, 1.0, 0.0)
    lower_b = lower.astype(BF16)
    stack[...] = jnp.zeros_like(stack)
    stack2[...] = jnp.ones_like(stack2)
    prefix[0] = jnp.zeros(prefix.shape[1:], F32)
    base[0:8] = jnp.zeros((8, channels), F32)
    state_out[...] = jnp.zeros_like(state_out)

    @pl.when(z == 0)
    def _():
        state_in[...] = jnp.zeros_like(state_in)

    loads[0].wait()
    loads[1].wait()
    for k in range(blocks):
        stack[k * padded : k * padded + heads, :] = log[:, k * BLOCK : (k + 1) * BLOCK]
        stack2[k * padded : k * padded + heads, :] = step[:, k * BLOCK : (k + 1) * BLOCK]
    rows_all, cols_all = 0.0, 0.0
    for part_of in split(stack[...], 3):
        rows_all = rows_all + dot(part_of, lower_b, 1, 1)
        cols_all = cols_all + dot(lower_b, part_of, 1, 1)
    steps = stack2[...]
    rows_ref[...] = rows_all - jnp.log(steps)
    to_end = jnp.exp(rows_all[:, BLOCK - 1 : BLOCK] - rows_all) * steps
    ends_ref[...] = to_end
    for k in range(blocks):
        cols_ref[k] = cols_all[:, k * padded : (k + 1) * padded]

    loads[2].wait()
    loads[3].wait()
    middle = (len(every) + 1) // 2
    for some in (every[:middle], every[middle:]):
        if not some:
            continue

        def state_step(k, carry, some=some):
            row = pl.ds(pl.multiple_of(k * BLOCK, BLOCK), BLOCK)
            spot = pl.ds(pl.multiple_of(k * 8, 8), 8)
            following = pl.ds(pl.multiple_of(k * 8 + 8, 8), 8)
            end = cols_ref[k, BLOCK - 8 : BLOCK, :][7:8, :]
            ends = ends_ref[pl.ds(pl.multiple_of(k * padded, padded), padded), :]
            turned = {}
            for p, start, width, of, group in some:
                lanes = slice(start, start + width)
                last = spread(end, of, width)
                if group not in turned:
                    turned[group] = b[row, group * STATE : (group + 1) * STATE].T.astype(F32)
                scaled = [(turned[group] * ends[head : head + 1, :]).astype(BF16) for head in of]
                both = dot(jnp.concatenate(scaled, axis=0), x[row, lanes], 1, 0)
                new = both[:STATE]
                if len(of) > 1:
                    new = jnp.where(iotas(STATE, width)[1] < HEAD_DIM, new, both[STATE:])
                prefix[k + 1, :, lanes] = jnp.exp(last) * prefix[k, :, lanes] + new
                base[following, lanes] = base[spot, lanes] + last
            return carry

        lax.fori_loop(0, blocks, state_step, 0)
        if S > 1:
            @pl.when(z == 0)
            def _(some=some):
                for p, start, width, of, group in some:
                    state_out[p, :, :width] = prefix[blocks, :, start : start + width].astype(BF16)
                    state_copy(p).start()

    def pass_state():
        for p, start, width, of, group in every:
            lanes = slice(start, start + width)
            state_copy(p).wait_recv()

            @pl.when(z < S - 1)
            def _():
                grown = jnp.exp(base[blocks * 8 : blocks * 8 + 1, lanes]) * state_in[p, :, :width].astype(F32)
                state_out[p, :, :width] = (grown + prefix[blocks, :, lanes]).astype(BF16)
                state_copy(p).start()

    def block_of(j):
        mixed = j < 2 * share_blocks
        rest = j - 2 * share_blocks
        dx = jnp.where(mixed, 1 - j % 2, 1 - rest // share_blocks)
        dy = jnp.where(mixed, 1, 0)
        sub = jnp.where(mixed, j // 2, rest % share_blocks)
        return dx, dy, sub

    def within(k):
        row = pl.ds(pl.multiple_of(k * BLOCK, BLOCK), BLOCK)
        mid = BLOCK // 2
        columns = cols_ref[k]
        rows = rows_ref[pl.ds(pl.multiple_of(k * padded, padded), padded), :]
        scores = {}
        for p, start, width, of, group in every:
            lanes = slice(start, start + width)
            if group not in scores:
                which = slice(group * STATE, (group + 1) * STATE)
                scores[group] = dot(c[row, which], b[row, which], 1, 1) * lower
            x_here = x[row, lanes]
            lane = iotas(BLOCK, width)[1]
            top, bottom = 0.0, 0.0
            for i, head in enumerate(of):
                kept = (lane >= i * HEAD_DIM) & (lane < (i + 1) * HEAD_DIM)
                x_head = x_here if len(of) == 1 else jnp.where(kept, x_here, jnp.zeros_like(x_here))
                column, across = columns[:, head : head + 1], rows[head : head + 1, :]
                w_top = scores[group][:mid, :mid] * jnp.exp(
                    jnp.minimum(column[:mid] - across[:, :mid], 0.0)
                )
                w_bottom = scores[group][mid:] * jnp.exp(jnp.minimum(column[mid:] - across, 0.0))
                top = top + dot(w_top.astype(BF16), x_head[:mid], 1, 0)
                bottom = bottom + dot(w_bottom.astype(BF16), x_head, 1, 0)
            gains = jnp.full((1, width), skip_ref[of[0]], F32)
            if len(of) > 1:
                gains = jnp.where(iotas(1, width)[1] < HEAD_DIM, gains, skip_ref[of[1]])
            direct = gains * x_here.astype(F32)
            x[row, lanes] = jnp.concatenate([top + direct[:mid], bottom + direct[mid:]], axis=0).astype(BF16)

    def row_of(dx, dy, sub):
        owner = ((gy + dy) % Y) * X + (gx + dx) % X
        return pl.multiple_of(owner * per_share + sub * unit, unit)

    def copy_gated(dy, sub):
        return pltpu.make_async_remote_copy(
            src_ref=x.at[pl.ds(row_of(1, dy, sub), unit), :], dst_ref=gated_in.at[dy, sub],
            send_sem=gated_send.at[dy, sub], recv_sem=gated_recv.at[dy, sub],
            device_id=to(1, 0), device_id_type=MESH,
        )

    def copy_squares(dx, dy, sub, index):
        slot = dx * Y + dy
        return pltpu.make_async_remote_copy(
            src_ref=squares.at[index], dst_ref=squares_in.at[slot, sub],
            send_sem=square_send.at[slot, sub], recv_sem=square_recv.at[slot, sub],
            device_id=to(dx, dy), device_id_type=MESH,
        )

    def copy_sums(sub, m):
        return pltpu.make_async_remote_copy(
            src_ref=sums_out.at[sub, m], dst_ref=sums_in.at[sub, m],
            send_sem=sums_send.at[sub, m], recv_sem=sums_recv.at[sub, m],
            device_id=to(0, 1), device_id_type=MESH,
        )

    def finish(j):
        dx, dy, part_of_share = block_of(j)
        k = row_of(dx, dy, part_of_share * units) // BLOCK
        row = pl.ds(pl.multiple_of(k * BLOCK, BLOCK), BLOCK)
        grow_all = jnp.exp(cols_ref[k])
        before = jnp.exp(base[pl.ds(pl.multiple_of(k * 8, 8), 8), :])
        total = {}
        for p, start, width, of, group in every:
            lanes = slice(start, start + width)
            entering = prefix[k, :, lanes] + before[0:1, lanes] * state_in[p, :, :width].astype(F32)
            moved = dot(c[row, group * STATE : (group + 1) * STATE], entering.astype(BF16), 1, 0)
            across = spread(grow_all, of, width) * moved
            v = gate[row, lanes].astype(F32)
            gated = (x[row, lanes].astype(F32) + across) * (v * (0.5 + 0.5 * jnp.tanh(0.5 * v)))
            total[width] = total.get(width, 0.0) + gated * gated
            x[row, lanes] = (gated * gain_ref[pl.ds(first_gain + p, 1), :width]).astype(BF16)
        summed = jnp.zeros((8, BLOCK), F32)
        for width, value in total.items():
            for part_of in split(value, 2):
                summed = summed + dot(jnp.ones((8, width), BF16), part_of, 1, 1)
        for u in range(units):
            squares[k * units + u] = summed[:, u * unit : (u + 1) * unit]

        @pl.when(dx > 0)
        def _():
            for u in range(units):
                copy_gated(dy, part_of_share * units + u).start()

        @pl.when(dx + dy > 0)
        def _():
            for u in range(units):
                copy_squares(dx, dy, part_of_share * units + u, k * units + u).start()

    def product(row, size, m, arrived):
        columns = pl.ds(pl.multiple_of(m * wide, wide), wide)
        return dot(x[pl.ds(row, size), :], w[:, columns], 1, 0) + dot(arrived, theirs[m], 1, 0)

    loads[4].wait()
    waits = jnp.where(z > 0, lax.min(z * blocks // (S - 1), blocks - 1), -1)

    def within_step(i, carry):
        within(i)

        @pl.when(i == waits)
        def _():
            pass_state()

        relay(i)
        return carry

    def finish_step(i, carry):
        finish(i)
        relay(i + blocks)
        return carry

    lax.fori_loop(0, blocks, within_step, 0)
    loads[5].wait()
    lax.fori_loop(0, blocks, finish_step, 0)
    loads[6].wait()

    def far_tiles(sub, first, last):
        def tile(position, carry):
            m = chunk_at(position)

            @pl.when(sub == 0)
            def _():
                w_arrival(m, 1 - core).wait_recv()

            sums_out[sub, m] = product(row_of(0, 1, sub), unit, m, gated_in[1, sub]).astype(BF16)
            copy_sums(sub, m).start()
            return carry

        lax.fori_loop(first, last, tile, 0)

    def of_step(at):
        found = jnp.int32(ready[0])
        for i in range(1, subs + 1):
            found = jnp.where(at >= i, jnp.int32(ready[i]), found)
        return found

    def far_step(sub, carry):
        copy_gated(1, sub).wait_recv()
        known = of_step(sub)
        far_tiles(sub, 0, known)
        relay(2 * blocks + sub)
        fresh = of_step(sub + 1)

        def older(other, carry):
            far_tiles(other, known, fresh)
            return carry

        lax.fori_loop(0, sub + 1, older, 0)
        return carry

    lax.fori_loop(0, subs, far_step, 0)

    def late_step(position, carry):
        relay(position, final)

        def older(other, carry):
            far_tiles(other, position, position + 1)
            return carry

        lax.fori_loop(0, subs, older, 0)
        return carry

    lax.fori_loop(ready[subs], count, late_step, 0)

    same_u = jnp.where(iotas(unit, unit)[0] == iotas(unit, unit)[1], 1.0, 0.0)

    def scale_step(sub, carry):
        summed = squares[me * subs + sub]
        for dx in range(X):
            for dy in range(Y):
                if dx + dy > 0:
                    copy_squares(dx, dy, sub, 0).wait_recv()
                    summed = summed + squares_in[dx * Y + dy, sub]
        column = dot(same_u, summed, 1, 1, HIGHEST)[:, 0:1]
        there = pl.ds(pl.multiple_of(sub * unit, unit), unit)
        scale_ref[there, :] = jnp.broadcast_to(lax.rsqrt(column / (HEAD_COUNT * HEAD_DIM) + epsilon), (unit, LANES))
        return carry

    lax.fori_loop(0, subs, scale_step, 0)

    def out_copy(block, m):
        there = pl.ds(pl.multiple_of(block * BLOCK, BLOCK), BLOCK)
        columns = pl.ds(pl.multiple_of(m * wide, wide), wide)
        return pltpu.make_async_copy(stage.at[there, columns], out_hbm.at[there, columns], out_sem.at[block, m])

    def near_tile(block, position):
        there = pl.ds(pl.multiple_of(block * BLOCK, BLOCK), BLOCK)
        m = chunk_at(position)
        columns = pl.ds(pl.multiple_of(m * wide, wide), wide)
        arrived = jnp.concatenate([gated_in[0, block * units + u] for u in range(units)], axis=0)
        value = product(row_of(0, 0, block * units), BLOCK, m, arrived)
        for u in range(units):
            copy_sums(block * units + u, m).wait_recv()
        value = value + jnp.concatenate([sums_in[block * units + u, m] for u in range(units)], axis=0).astype(F32)
        scale = scale_ref[there, :]
        stage[there, columns] = (value * jnp.concatenate([scale, scale], axis=1)).astype(BF16)
        out_copy(block, m).start()

    def near_step(block, carry):
        for u in range(units):
            copy_gated(0, block * units + u).wait_recv()

        def tile(position, carry):
            near_tile(block, position)
            return carry

        lax.fori_loop(0, ready[subs], tile, 0)
        return carry

    def last_step(i, carry):
        near_tile(i % share_blocks, ready[subs] + i // share_blocks)
        return carry

    lax.fori_loop(0, share_blocks, near_step, 0)
    lax.fori_loop(0, share_blocks * (count - ready[subs]), last_step, 0)

    def drain(m, carry):
        for sub in range(subs):
            copy_sums(sub, m).wait_send()
        for block in range(share_blocks):
            out_copy(block, m).wait()
        w_copy(m, "side").wait_send()
        return carry

    lax.fori_loop(0, count, drain, 0)
    for sub in range(subs):
        for dy in range(Y):
            copy_gated(dy, sub).wait_send()
        for dx in range(X):
            for dy in range(Y):
                if dx + dy > 0:
                    copy_squares(dx, dy, sub, 0).wait_send()
    for zz in range(S):
        @pl.when(z == zz)
        def _(zz=zz):
            for m in range(count):
                if homes[m] == zz:
                    w_copy(m, "first").wait_send()
                if zz > 0 and homes[m] >= zz:
                    w_copy(m, "left").wait_send()
                if zz < S - 1 and homes[m] <= zz:
                    w_copy(m, "right").wait_send()

    @pl.when(z < S - 1)
    def _():
        for p, start, width, of, group in every:
            state_copy(p).wait_send()


def body(
    ssm_input, gate_input, b_proj, c_proj, step_size, log_decay, skip_gain, norm_gain, out_weight
):
    tokens, channels = ssm_input.shape
    heads = step_size.shape[0]
    blocks = tokens // BLOCK
    model = out_weight.shape[1]
    half = model // 2
    per_group = HEAD_COUNT // GROUPS
    groups = max(1, heads // per_group)
    repeats = min(heads, per_group)
    H = lax.axis_size("head")
    S = lax.axis_size("seq")
    X = max(d for d in range(1, H + 1) if H % d == 0 and d * d <= H)
    Y = H // X
    per_share = tokens // H
    unit = min(UNIT, per_share)
    subs = per_share // unit
    count = len(pieces(channels, repeats))
    padded = -(-heads // 8) * 8
    head_index = lax.axis_index("head")
    gain = norm_gain
    if channels % LANES != 0:
        gain = lax.dynamic_slice_in_dim(norm_gain, head_index * channels, channels)
        gain = jnp.pad(gain, (0, count * LANES - channels))
    gain = gain.reshape(-1, LANES)
    anywhere = pl.BlockSpec(memory_space=pl.ANY)
    vmem = pl.BlockSpec(memory_space=pltpu.VMEM)
    dma = pltpu.SemaphoreType.DMA
    x1, y1 = max(X - 1, 1), max(Y - 1, 1)
    side = [anywhere] * 6 + [pl.BlockSpec(memory_space=pltpu.SMEM), vmem, anywhere]
    paired = (
        X == 2 and Y == 2 and S > 1 and lax.axis_size("batch") == 2 and per_share % BLOCK == 0
        and model % (2 * LANES) == 0 and channels % LANES == 0 and model // (2 * LANES) >= S
        and per_share == 4 * UNIT
    )
    common = [
        pltpu.VMEM((tokens, channels), BF16),
        pltpu.VMEM((tokens, channels), BF16),
        pltpu.VMEM((tokens, groups * STATE), BF16),
        pltpu.VMEM((tokens, groups * STATE), BF16),
        pltpu.VMEM((heads, tokens), F32),
        pltpu.VMEM((heads, tokens), F32),
        pltpu.VMEM((channels, model), BF16),
        pltpu.VMEM((blocks * padded, BLOCK), F32),
        pltpu.VMEM((blocks * padded, BLOCK), F32),
        pltpu.VMEM((blocks * padded, BLOCK), F32),
        pltpu.VMEM((blocks, BLOCK, padded), F32),
        pltpu.VMEM((blocks * padded, BLOCK), F32),
        pltpu.VMEM((blocks + 1, STATE, channels), F32),
        pltpu.VMEM(((blocks + 1) * 8, channels), F32),
        pltpu.VMEM((count, STATE, LANES), BF16),
        pltpu.VMEM((count, STATE, LANES), BF16),
    ]
    cost = pl.CostEstimate(
        flops=2 * tokens * channels * (model + 4 * BLOCK), bytes_accessed=tokens * channels * 8, transcendentals=0
    )
    params = pltpu.CompilerParams(
        collective_id=0, has_side_effects=True, vmem_limit_bytes=62 * 1024 * 1024
    )
    if paired:
        tiles = model // (2 * LANES)
        return pl.pallas_call(
            functools.partial(pair_kernel, (X, Y, S, groups, repeats)),
            in_specs=side,
            out_specs=anywhere,
            out_shape=jax.ShapeDtypeStruct((per_share, model), BF16),
            scratch_shapes=common + [
                pltpu.VMEM((tiles, channels, 2 * LANES), BF16),
                pltpu.VMEM((tokens // unit, 8, unit), F32),
                pltpu.VMEM((H, subs, 8, unit), F32),
                pltpu.VMEM((Y, subs, unit, channels), BF16),
                pltpu.VMEM((subs, tiles, unit, 2 * LANES), BF16),
                pltpu.VMEM((subs, tiles, unit, 2 * LANES), BF16),
                pltpu.VMEM((per_share, model), BF16),
                pltpu.VMEM((per_share, LANES), F32),
                dma((7,)),
                dma((per_share // BLOCK, tiles)),
                dma((count,)),
                dma((count,)),
                dma((H, subs)),
                dma((H, subs)),
                dma((4, tiles)),
                dma((tiles, 2)),
                dma((Y, subs)),
                dma((Y, subs)),
                dma((subs, tiles)),
                dma((subs, tiles)),
            ],
            compiler_params=params,
            name="mixer_pair",
            cost_estimate=cost,
        )(ssm_input, gate_input, b_proj, c_proj, step_size, log_decay, skip_gain, gain, out_weight)
    return pl.pallas_call(
        functools.partial(mixer_kernel, (X, Y, S, groups, repeats)),
        in_specs=side,
        out_specs=anywhere,
        out_shape=jax.ShapeDtypeStruct((per_share, model), BF16),
        scratch_shapes=common + [
            pltpu.VMEM((BLOCK, channels), BF16),
            pltpu.VMEM((tokens, model), BF16),
            pltpu.VMEM((tokens // unit, 8, unit), F32),
            pltpu.VMEM((H, subs, 8, unit), F32),
            pltpu.VMEM((x1, Y, subs, unit, half), BF16),
            pltpu.VMEM((y1, X, subs, unit, model - half), BF16),
            pltpu.VMEM((y1, subs, unit, half), BF16),
            pltpu.VMEM((x1, subs, unit, model - half), BF16),
            pltpu.VMEM((per_share, model), BF16),
            dma((7,)),
            dma((subs,)),
            dma((count,)),
            dma((count,)),
            dma((H, subs)),
            dma((H, subs)),
            dma((x1, Y, subs)),
            dma((x1, Y, subs)),
            dma((y1, X, subs)),
            dma((y1, X, subs)),
            dma((y1, subs)),
            dma((y1, subs)),
            dma((x1, subs)),
            dma((x1, subs)),
        ],
        compiler_params=params,
        name="mixer",
        cost_estimate=cost,
    )(ssm_input, gate_input, b_proj, c_proj, step_size, log_decay, skip_gain, gain, out_weight)


def solution(mesh):
    in_specs = (
        P(("batch", "seq"), "head"),
        P(("batch", "seq"), "head"),
        P(("batch", "seq"), None),
        P(("batch", "seq"), None),
        P("head", ("batch", "seq")),
        P("head", ("batch", "seq")),
        P("head"),
        P(),
        P("head", None),
    )
    out_specs = P(("batch", "seq", "head"), None)
    return jax.shard_map(body, mesh=mesh, in_specs=in_specs, out_specs=out_specs, check_vma=False)
```

```python
import functools
import jax
import jax.numpy as jnp
from jax import lax
from jax.experimental import pallas as pl
from jax.experimental.pallas import tpu as pltpu
from jax.sharding import PartitionSpec as P

HEAD_COUNT = 80
HEAD_DIM = 64
STATE = 128
GROUPS = 8
BLOCK = 256
LANES = 128
UNIT = 128
epsilon = 1e-05
HIGHEST = lax.Precision.HIGHEST
F32 = jnp.float32
BF16 = jnp.bfloat16
MESH = pl.DeviceIdType.MESH


def dot(a, b, ca, cb, precision=None):
    return lax.dot_general(
        a, b, (((ca,), (cb,)), ((), ())), precision=precision, preferred_element_type=F32
    )


def iotas(rows, columns):
    return (
        lax.broadcasted_iota(jnp.int32, (rows, columns), 0),
        lax.broadcasted_iota(jnp.int32, (rows, columns), 1),
    )


def pieces(channels, repeats):
    found = []
    for start in range(0, channels, LANES):
        width = min(LANES, channels - start)
        heads = [start // HEAD_DIM + i for i in range(width // HEAD_DIM)]
        found.append((len(found), start, width, heads, heads[0] // repeats))
    return found


def spread(columns, heads, width):
    rows = columns.shape[0]
    first = jnp.broadcast_to(columns[:, heads[0] : heads[0] + 1], (rows, width))
    if len(heads) == 1:
        return first
    second = jnp.broadcast_to(columns[:, heads[1] : heads[1] + 1], (rows, width))
    lane = iotas(rows, width)[1]
    return jnp.where(lane < HEAD_DIM, first, second)


def split(value, count):
    parts = []
    for _ in range(count):
        part = value.astype(BF16)
        parts.append(part)
        value = value - part.astype(F32)
    return parts


def column_tiles(start, stop, size):
    return [(at, min(size, stop - at)) for at in range(start, stop, size)]


def mixer_kernel(
    plan, x_hbm, gate_hbm, b_hbm, c_hbm, step_hbm, log_hbm, skip_ref, gain_ref, w_hbm, out_hbm,
    x, gate, b, c, step, log, w, stack, stack2, rows_ref, cols_ref, ends_ref, prefix, base,
    state_out, state_in, g_ref, part, squares, squares_in, first_a, first_b, second_a, second_b, stage,
    load_sem, out_sem, state_send, state_recv, square_send, square_recv,
    first_a_send, first_a_recv, first_b_send, first_b_recv,
    second_a_send, second_a_recv, second_b_send, second_b_recv,
):
    X, Y, S, groups, repeats = plan
    H = X * Y
    tokens, channels = x.shape
    model = w.shape[1]
    half = model // 2
    heads = step.shape[0]
    padded = stack.shape[0] // (tokens // BLOCK)
    blocks = tokens // BLOCK
    per_share = tokens // H
    unit = min(UNIT, per_share)
    subs = per_share // unit
    units = BLOCK // unit
    per_group = HEAD_COUNT // GROUPS
    every = pieces(channels, repeats)
    first_gain = lax.axis_index("head") * len(every) if channels % LANES == 0 else 0

    me = lax.axis_index("head")
    z = lax.axis_index("seq")
    gx = me % X
    gy = me // X
    to = lambda dx, dy: {"head": ((gy + dy) % Y) * X + (gx + dx) % X}
    after = {"seq": lax.rem(z + 1, S)}

    offset = pl.multiple_of((me * heads // per_group) // groups * (groups * STATE), STATE)
    loads = [
        pltpu.make_async_copy(log_hbm, log, load_sem.at[0]),
        pltpu.make_async_copy(step_hbm, step, load_sem.at[1]),
        pltpu.make_async_copy(b_hbm.at[:, pl.ds(offset, groups * STATE)], b, load_sem.at[2]),
        pltpu.make_async_copy(x_hbm, x, load_sem.at[3]),
        pltpu.make_async_copy(c_hbm.at[:, pl.ds(offset, groups * STATE)], c, load_sem.at[4]),
        pltpu.make_async_copy(gate_hbm, gate, load_sem.at[5]),
        pltpu.make_async_copy(w_hbm, w, load_sem.at[6]),
    ]
    for load in loads:
        load.start()

    barrier = pltpu.get_barrier_semaphore()
    for d in range(1, H):
        pl.semaphore_signal(barrier, inc=1, device_id={"head": lax.rem(me + d, H)}, device_id_type=MESH)
    if S > 1:
        @pl.when(z > 0)
        def _():
            pl.semaphore_signal(barrier, inc=1, device_id={"seq": lax.max(z - 1, 0)}, device_id_type=MESH)

        @pl.when(z < S - 1)
        def _():
            pl.semaphore_signal(barrier, inc=1, device_id=after, device_id_type=MESH)

    near = 0
    if S > 1:
        near = jnp.where(z > 0, 1, 0) + jnp.where(z < S - 1, 1, 0)
    pl.semaphore_wait(barrier, near + (H - 1))

    def state_copy(p):
        return pltpu.make_async_remote_copy(
            src_ref=state_out.at[p], dst_ref=state_in.at[p], send_sem=state_send.at[p],
            recv_sem=state_recv.at[p], device_id=after, device_id_type=MESH,
        )

    t_iota, s_iota = iotas(BLOCK, BLOCK)
    lower = jnp.where(s_iota <= t_iota, 1.0, 0.0)
    lower_b = lower.astype(BF16)
    stack[...] = jnp.zeros_like(stack)
    stack2[...] = jnp.ones_like(stack2)
    prefix[0] = jnp.zeros(prefix.shape[1:], F32)
    base[0:8] = jnp.zeros((8, channels), F32)
    state_out[...] = jnp.zeros_like(state_out)

    @pl.when(z == 0)
    def _():
        state_in[...] = jnp.zeros_like(state_in)

    loads[0].wait()
    loads[1].wait()
    for k in range(blocks):
        stack[k * padded : k * padded + heads, :] = log[:, k * BLOCK : (k + 1) * BLOCK]
        stack2[k * padded : k * padded + heads, :] = step[:, k * BLOCK : (k + 1) * BLOCK]
    rows_all, cols_all = 0.0, 0.0
    for part_of in split(stack[...], 3):
        rows_all = rows_all + dot(part_of, lower_b, 1, 1)
        cols_all = cols_all + dot(lower_b, part_of, 1, 1)
    steps = stack2[...]
    rows_ref[...] = rows_all - jnp.log(steps)
    to_end = jnp.exp(rows_all[:, BLOCK - 1 : BLOCK] - rows_all) * steps
    ends_ref[...] = to_end
    for k in range(blocks):
        cols_ref[k] = cols_all[:, k * padded : (k + 1) * padded]

    loads[2].wait()
    loads[3].wait()
    middle = (len(every) + 1) // 2
    for some in (every[:middle], every[middle:]):
        if not some:
            continue

        def state_step(k, carry, some=some):
            row = pl.ds(pl.multiple_of(k * BLOCK, BLOCK), BLOCK)
            spot = pl.ds(pl.multiple_of(k * 8, 8), 8)
            following = pl.ds(pl.multiple_of(k * 8 + 8, 8), 8)
            end = cols_ref[k, BLOCK - 8 : BLOCK, :][7:8, :]
            ends = ends_ref[pl.ds(pl.multiple_of(k * padded, padded), padded), :]
            turned = {}
            for p, start, width, of, group in some:
                lanes = slice(start, start + width)
                last = spread(end, of, width)
                if group not in turned:
                    turned[group] = b[row, group * STATE : (group + 1) * STATE].T.astype(F32)
                scaled = [(turned[group] * ends[head : head + 1, :]).astype(BF16) for head in of]
                both = dot(jnp.concatenate(scaled, axis=0), x[row, lanes], 1, 0)
                new = both[:STATE]
                if len(of) > 1:
                    new = jnp.where(iotas(STATE, width)[1] < HEAD_DIM, new, both[STATE:])
                prefix[k + 1, :, lanes] = jnp.exp(last) * prefix[k, :, lanes] + new
                base[following, lanes] = base[spot, lanes] + last
            return carry

        lax.fori_loop(0, blocks, state_step, 0)
        if S > 1:
            @pl.when(z == 0)
            def _(some=some):
                for p, start, width, of, group in some:
                    state_out[p, :, :width] = prefix[blocks, :, start : start + width].astype(BF16)
                    state_copy(p).start()

    def pass_state():
        for p, start, width, of, group in every:
            lanes = slice(start, start + width)
            state_copy(p).wait_recv()

            @pl.when(z < S - 1)
            def _():
                grown = jnp.exp(base[blocks * 8 : blocks * 8 + 1, lanes]) * state_in[p, :, :width].astype(F32)
                state_out[p, :, :width] = (grown + prefix[blocks, :, lanes]).astype(BF16)
                state_copy(p).start()

    def block_of(j):
        if per_share < BLOCK:
            return j
        chunks = per_share // BLOCK
        o = j // chunks
        dx = X - 1 - o // Y
        dy = Y - 1 - o % Y
        return (((gy + dy) % Y) * X + (gx + dx) % X) * chunks + j % chunks

    def within(j):
        k = block_of(j)
        row = pl.ds(pl.multiple_of(k * BLOCK, BLOCK), BLOCK)
        mid = BLOCK // 2
        columns = cols_ref[k]
        rows = rows_ref[pl.ds(pl.multiple_of(k * padded, padded), padded), :]
        scores = {}
        for p, start, width, of, group in every:
            lanes = slice(start, start + width)
            if group not in scores:
                which = slice(group * STATE, (group + 1) * STATE)
                scores[group] = dot(c[row, which], b[row, which], 1, 1) * lower
            x_here = x[row, lanes]
            lane = iotas(BLOCK, width)[1]
            top, bottom = 0.0, 0.0
            for i, head in enumerate(of):
                kept = (lane >= i * HEAD_DIM) & (lane < (i + 1) * HEAD_DIM)
                x_head = x_here if len(of) == 1 else jnp.where(kept, x_here, jnp.zeros_like(x_here))
                column, across = columns[:, head : head + 1], rows[head : head + 1, :]
                w_top = scores[group][:mid, :mid] * jnp.exp(
                    jnp.minimum(column[:mid] - across[:, :mid], 0.0)
                )
                w_bottom = scores[group][mid:] * jnp.exp(jnp.minimum(column[mid:] - across, 0.0))
                top = top + dot(w_top.astype(BF16), x_head[:mid], 1, 0)
                bottom = bottom + dot(w_bottom.astype(BF16), x_head, 1, 0)
            gains = jnp.full((1, width), skip_ref[of[0]], F32)
            if len(of) > 1:
                gains = jnp.where(iotas(1, width)[1] < HEAD_DIM, gains, skip_ref[of[1]])
            direct = gains * x_here.astype(F32)
            x[row, lanes] = jnp.concatenate([top + direct[:mid], bottom + direct[mid:]], axis=0).astype(BF16)

    def first_copy(buffer, send, recv, dx, dy, sub, row, columns, slot):
        return pltpu.make_async_remote_copy(
            src_ref=part.at[pl.ds(row, unit), columns],
            dst_ref=buffer.at[slot[0], slot[1], sub],
            send_sem=send.at[slot[0], slot[1], sub],
            recv_sem=recv.at[slot[0], slot[1], sub],
            device_id=to(dx, dy), device_id_type=MESH,
        )

    def copy_a(dx, dy, sub, row):
        return first_copy(
            first_a, first_a_send, first_a_recv, dx, 0, sub, row, pl.ds(0, half), (dx - 1, dy)
        )

    def copy_b(dx, dy, sub, row):
        return first_copy(
            first_b, first_b_send, first_b_recv, 0, dy, sub, row, pl.ds(half, model - half), (dy - 1, dx)
        )

    def copy_squares(dx, dy, sub, index):
        slot = dx * Y + dy
        return pltpu.make_async_remote_copy(
            src_ref=squares.at[index], dst_ref=squares_in.at[slot, sub],
            send_sem=square_send.at[slot, sub], recv_sem=square_recv.at[slot, sub],
            device_id=to(dx, dy), device_id_type=MESH,
        )

    def finish(j):
        k = block_of(j)
        row = pl.ds(pl.multiple_of(k * BLOCK, BLOCK), BLOCK)
        grow_all = jnp.exp(cols_ref[k])
        before = jnp.exp(base[pl.ds(pl.multiple_of(k * 8, 8), 8), :])
        total = {}
        for p, start, width, of, group in every:
            lanes = slice(start, start + width)
            entering = prefix[k, :, lanes] + before[0:1, lanes] * state_in[p, :, :width].astype(F32)
            moved = dot(c[row, group * STATE : (group + 1) * STATE], entering.astype(BF16), 1, 0)
            across = spread(grow_all, of, width) * moved
            v = gate[row, lanes].astype(F32)
            gated = (x[row, lanes].astype(F32) + across) * (v * (0.5 + 0.5 * jnp.tanh(0.5 * v)))
            total[width] = total.get(width, 0.0) + gated * gated
            g_ref[:, lanes] = (gated * gain_ref[pl.ds(first_gain + p, 1), :width]).astype(BF16)
        summed = jnp.zeros((8, BLOCK), F32)
        for width, value in total.items():
            for part_of in split(value, 2):
                summed = summed + dot(jnp.ones((8, width), BF16), part_of, 1, 1)
        for u in range(units):
            squares[k * units + u] = summed[:, u * unit : (u + 1) * unit]
        where = []
        for u in range(units):
            begin = pl.multiple_of(k * BLOCK + u * unit, unit)
            owner = begin // per_share
            sub = (begin % per_share) // unit
            where.append(((owner % X - gx + X) % X, (owner // X - gy + Y) % Y, sub, begin, k * units + u))
        for start, width in column_tiles(0, half, 512):
            part[row, start : start + width] = dot(g_ref[...], w[:, start : start + width], 1, 0).astype(BF16)
        for dx, dy, sub, begin, index in where:
            @pl.when(dx > 0)
            def _():
                copy_a(dx, dy, sub, begin).start()
        for start, width in column_tiles(half, model, 512):
            part[row, start : start + width] = dot(g_ref[...], w[:, start : start + width], 1, 0).astype(BF16)
        for dx, dy, sub, begin, index in where:
            @pl.when(dy > 0)
            def _():
                copy_b(dx, dy, sub, begin).start()

            @pl.when(dx + dy > 0)
            def _():
                copy_squares(dx, dy, sub, index).start()

    loads[4].wait()
    waits = jnp.where(z > 0, lax.min(z * blocks // (S - 1), blocks - 1), -1) if S > 1 else None

    def within_step(i, carry):
        within(i)
        if S > 1:
            @pl.when(i == waits)
            def _():
                pass_state()

        return carry

    def finish_step(i, carry):
        finish(i)
        return carry

    lax.fori_loop(0, blocks, within_step, 0)
    loads[5].wait()
    loads[6].wait()
    lax.fori_loop(0, blocks, finish_step, 0)

    def second_copy(buffer, send, recv, dx, dy, slot, sub, row, columns):
        return pltpu.make_async_remote_copy(
            src_ref=part.at[pl.ds(row, unit), columns], dst_ref=buffer.at[slot, sub],
            send_sem=send.at[slot, sub], recv_sem=recv.at[slot, sub],
            device_id=to(dx, dy), device_id_type=MESH,
        )

    left, right = pl.ds(0, half), pl.ds(half, model - half)

    def row_of(dx, dy, sub):
        owner = ((gy + dy) % Y) * X + (gx + dx) % X
        return pl.multiple_of(owner * per_share + sub * unit, unit)

    second_a_copy = lambda dy, sub: second_copy(
        second_a, second_a_send, second_a_recv, 0, dy, dy - 1, sub, row_of(0, dy, sub), left
    )
    second_b_copy = lambda dx, sub: second_copy(
        second_b, second_b_send, second_b_recv, dx, 0, dx - 1, sub, row_of(dx, 0, sub), right
    )

    def partial_sum(row, columns, buffer, copy, count, other, sub):
        value = part[pl.ds(row, unit), columns].astype(F32)
        for d in range(1, count):
            copy(d, other, sub, row).wait_recv()
            value = value + buffer[d - 1, other, sub].astype(F32)
        return value

    swapped_b = lambda dy, dx, sub, row: copy_b(dx, dy, sub, row)

    def relay(sub, carry):
        for dy in range(1, Y):
            row = row_of(0, dy, sub)
            part[pl.ds(row, unit), left] = partial_sum(row, left, first_a, copy_a, X, dy, sub).astype(BF16)
            second_a_copy(dy, sub).start()
        for dx in range(1, X):
            row = row_of(dx, 0, sub)
            part[pl.ds(row, unit), right] = partial_sum(row, right, first_b, swapped_b, Y, dx, sub).astype(BF16)
            second_b_copy(dx, sub).start()
        return carry

    lax.fori_loop(0, subs, relay, 0)

    def out_copy(sub):
        there = pl.ds(pl.multiple_of(sub * unit, unit), unit)
        return pltpu.make_async_copy(stage.at[there, :], out_hbm.at[there, :], out_sem.at[sub])

    same_u = jnp.where(iotas(unit, unit)[0] == iotas(unit, unit)[1], 1.0, 0.0)

    def settle(sub, carry):
        row = row_of(0, 0, sub)
        there = pl.ds(pl.multiple_of(sub * unit, unit), unit)
        summed = squares[me * subs + sub]
        for dx in range(X):
            for dy in range(Y):
                if dx + dy > 0:
                    copy_squares(dx, dy, sub, 0).wait_recv()
                    summed = summed + squares_in[dx * Y + dy, sub]
        column = dot(same_u, summed, 1, 1, HIGHEST)[:, 0:1]
        scale = lax.rsqrt(column / (HEAD_COUNT * HEAD_DIM) + epsilon)
        value = partial_sum(row, left, first_a, copy_a, X, 0, sub)
        for dy in range(1, Y):
            second_a_copy(dy, sub).wait_recv()
            value = value + second_a[dy - 1, sub].astype(F32)
        stage[there, left] = (value * scale).astype(BF16)
        value = partial_sum(row, right, first_b, swapped_b, Y, 0, sub)
        for dx in range(1, X):
            second_b_copy(dx, sub).wait_recv()
            value = value + second_b[dx - 1, sub].astype(F32)
        stage[there, right] = (value * scale).astype(BF16)
        out_copy(sub).start()
        return carry

    lax.fori_loop(0, subs, settle, 0)

    def drain(sub, carry):
        for dx in range(X):
            for dy in range(Y):
                if dx > 0:
                    copy_a(dx, dy, sub, 0).wait_send()
                if dy > 0:
                    copy_b(dx, dy, sub, 0).wait_send()
                if dx + dy > 0:
                    copy_squares(dx, dy, sub, 0).wait_send()
        for dy in range(1, Y):
            second_a_copy(dy, sub).wait_send()
        for dx in range(1, X):
            second_b_copy(dx, sub).wait_send()
        out_copy(sub).wait()
        return carry

    lax.fori_loop(0, subs, drain, 0)
    if S > 1:
        @pl.when(z < S - 1)
        def _():
            for p, start, width, of, group in every:
                state_copy(p).wait_send()


def relay_plan(homes, S, blocks, lag, passes):
    count = len(homes)
    span, hop = 7.5, 1.5
    steps = blocks + lag
    clock = [[0.0] * (steps + 4) for _ in range(S)]
    for z in range(S):
        now = 8.5
        for at in range(steps):
            now = now + (1.4 if at < blocks else 0.0) + (1.1 if at >= lag else 0.0)
            if z > 0 and at == passes[z]:
                now = max(now, 9.0 + 3.2 * z)
            if at == lag - 1:
                now = max(now, 9.0 + 3.2 * (S - 1))
            clock[z][at] = now
        for at in range(steps, steps + 4):
            now = now + (3.0 if at == steps else 7.5)
            clock[z][at] = now
    arrival = [[None] * count for _ in range(S)]
    taken = [{} for _ in range(S)]
    plan = [{} for _ in range(S)]
    order = [[] for _ in range(S)]
    free = {}
    for z in range(S):
        for r, m in enumerate(m for m in range(count) if homes[m] == z):
            arrival[z][m] = 2.5 + span * (r + 1)

    def send(z, m, when, step):
        begin = max(when, free.get((z, step), 0.0))
        free[z, step] = begin + span
        arrival[z + step][m] = begin + span + hop

    late = [[] for _ in range(S)]
    events = sorted((clock[z][at], z, at) for z in range(S) for at in range(steps + 4))
    for when, z, at in events:
        todo = plan[z].setdefault(at, [])
        if z == 0 or at > passes[z]:
            for m in late[z]:
                todo.append(("right", m))
                send(z, m, when, 1)
            late[z] = []
        ready = [m for m in range(count) if m not in taken[z] and arrival[z][m] is not None]
        ready = [m for m in ready if arrival[z][m] <= when + 0.2]
        for m in sorted(ready, key=lambda m: arrival[z][m]):
            taken[z][m] = at
            order[z].append(m)
            todo.append(("take", m))
            todo.append(("side", m))
            if z > 0 and homes[m] >= z:
                todo.append(("left", m))
                send(z, m, when, -1)
            if z < S - 1 and homes[m] <= z:
                if z == 0 or at > passes[z]:
                    todo.append(("right", m))
                    send(z, m, when, 1)
                else:
                    late[z].append(m)
    final = [{} for _ in range(S)]
    for z in range(S):
        rest = [m for m in range(count) if m not in taken[z]]
        for m in sorted(rest, key=lambda m: (abs(homes[m] - z), m)):
            todo = final[z].setdefault(len(order[z]), [("take", m), ("side", m)])
            order[z].append(m)
            if z > 0 and homes[m] >= z:
                todo.append(("left", m))
            if z < S - 1 and homes[m] <= z:
                todo.append(("right", m))
    ready = [
        min(sum(1 for m in taken[z] if taken[z][m] < at) for z in range(S))
        for at in range(steps, steps + 5)
    ]
    return plan, final, order, ready


def home_planes(count, S):
    sizes = [count // S] * S
    ends = [z for i in range(S) for z in ({i, S - 1 - i} if i < S - 1 - i else {i})][:S]
    for i in range(count % S):
        sizes[ends[i]] += 1
    return [z for z in range(S) for _ in range(sizes[z])]


def pair_kernel(
    plan, x_hbm, gate_hbm, b_hbm, c_hbm, step_hbm, log_hbm, skip_ref, gain_ref, w_hbm, out_hbm,
    x, gate, b, c, step, log, w, stack, stack2, rows_ref, cols_ref, ends_ref, prefix, base,
    state_out, state_in, theirs, squares, squares_in, gated_in, sums_out, sums_in, stage, scale_ref, own_ref,
    load_sem, out_sem, state_send, state_recv, square_send, square_recv,
    w_send, w_recv, gated_send, gated_recv, sums_send, sums_recv,
):
    X, Y, S, groups, repeats = plan
    H = X * Y
    tokens, channels = x.shape
    model = w.shape[1]
    heads = step.shape[0]
    blocks = tokens // BLOCK
    padded = stack.shape[0] // blocks
    per_share = tokens // H
    unit = UNIT
    subs = per_share // unit
    units = BLOCK // unit
    share_blocks = per_share // BLOCK
    per_group = HEAD_COUNT // GROUPS
    every = pieces(channels, repeats)
    first_gain = lax.axis_index("head") * len(every)
    wide = 2 * LANES
    count = model // wide
    homes = home_planes(count, S)
    passes = [max(zz * blocks // S - 1, 0) for zz in range(S)]
    lag = passes[-1] + 1
    tasks, final, order, ready = relay_plan(homes, S, blocks, lag, passes)

    me = lax.axis_index("head")
    z = lax.axis_index("seq")
    core = lax.axis_index("batch")
    gx = me % X
    gy = me // X
    to = lambda dx, dy: {"head": ((gy + dy) % Y) * X + (gx + dx) % X}
    after = {"seq": lax.rem(z + 1, S)}
    prior = {"seq": lax.max(z - 1, 0)}
    sibling = {"batch": 1 - core}

    offset = pl.multiple_of((me * heads // per_group) // groups * (groups * STATE), STATE)
    loads = [
        pltpu.make_async_copy(log_hbm, log, load_sem.at[0]),
        pltpu.make_async_copy(step_hbm, step, load_sem.at[1]),
        pltpu.make_async_copy(b_hbm.at[:, pl.ds(offset, groups * STATE)], b, load_sem.at[2]),
        pltpu.make_async_copy(x_hbm, x, load_sem.at[3]),
        pltpu.make_async_copy(c_hbm.at[:, pl.ds(offset, groups * STATE)], c, load_sem.at[4]),
        pltpu.make_async_copy(gate_hbm, gate, load_sem.at[5]),
        pltpu.make_async_copy(w_hbm, w, load_sem.at[6]),
    ]
    for load in loads[:4]:
        load.start()

    barrier = pltpu.get_barrier_semaphore()
    for d in range(1, H):
        pl.semaphore_signal(barrier, inc=1, device_id={"head": lax.rem(me + d, H)}, device_id_type=MESH)
    pl.semaphore_signal(barrier, inc=1, device_id=sibling, device_id_type=MESH)

    @pl.when(z > 0)
    def _():
        pl.semaphore_signal(barrier, inc=1, device_id=prior, device_id_type=MESH)

    @pl.when(z < S - 1)
    def _():
        pl.semaphore_signal(barrier, inc=1, device_id=after, device_id_type=MESH)

    pl.semaphore_wait(barrier, jnp.where(z > 0, 1, 0) + jnp.where(z < S - 1, 1, 0) + H)

    def held(m, which):
        return theirs.at[m, :, pl.ds(pl.multiple_of(which * LANES, LANES), LANES)]

    def w_copy(m, kind):
        source = held(m, core)
        if kind == "first":
            source = w_hbm.at[:, pl.ds(pl.multiple_of(m * wide + core * LANES, LANES), LANES)]
        return pltpu.make_async_remote_copy(
            src_ref=source, dst_ref=held(m, core),
            send_sem=w_send.at[("first", "side", "left", "right").index(kind), m],
            recv_sem=w_recv.at[m, core],
            device_id={"first": to(1, 0), "side": sibling, "left": prior, "right": after}[kind],
            device_id_type=MESH,
        )

    def w_arrival(m, which):
        return pltpu.make_async_remote_copy(
            src_ref=held(m, which), dst_ref=held(m, which), send_sem=w_send.at[0, m],
            recv_sem=w_recv.at[m, which], device_id=sibling, device_id_type=MESH,
        )

    for zz in range(S):
        @pl.when(z == zz)
        def _(zz=zz):
            for m in range(count):
                if homes[m] == zz:
                    w_copy(m, "first").start()

    def relay(at, tasks=tasks):
        for zz in range(S):
            @pl.when(z == zz)
            def _(zz=zz):
                for slot, todo in tasks[zz].items():
                    if not todo:
                        continue

                    @pl.when(at == slot)
                    def _(todo=todo):
                        for kind, m in todo:
                            if kind == "take":
                                w_arrival(m, core).wait_recv()
                            else:
                                w_copy(m, kind).start()

    def chunk_at(position):
        found = jnp.int32(0)
        for zz in range(S):
            for at in range(count):
                found = jnp.where((z == zz) & (position == at), order[zz][at], found)
        return found

    def state_copy(p):
        return pltpu.make_async_remote_copy(
            src_ref=state_out.at[p], dst_ref=state_in.at[p], send_sem=state_send.at[p],
            recv_sem=state_recv.at[p], device_id=after, device_id_type=MESH,
        )

    t_iota, s_iota = iotas(BLOCK, BLOCK)
    lower = jnp.where(s_iota <= t_iota, 1.0, 0.0)
    lower_b = lower.astype(BF16)
    stack[...] = jnp.zeros_like(stack)
    stack2[...] = jnp.ones_like(stack2)
    prefix[0] = jnp.zeros(prefix.shape[1:], F32)
    base[0:8] = jnp.zeros((8, channels), F32)
    state_out[...] = jnp.zeros_like(state_out)

    @pl.when(z == 0)
    def _():
        state_in[...] = jnp.zeros_like(state_in)

    loads[0].wait()
    loads[1].wait()
    for k in range(blocks):
        stack[k * padded : k * padded + heads, :] = log[:, k * BLOCK : (k + 1) * BLOCK]
        stack2[k * padded : k * padded + heads, :] = step[:, k * BLOCK : (k + 1) * BLOCK]
    rows_all, cols_all = 0.0, 0.0
    for part_of in split(stack[...], 3):
        rows_all = rows_all + dot(part_of, lower_b, 1, 1)
        cols_all = cols_all + dot(lower_b, part_of, 1, 1)
    steps = stack2[...]
    rows_ref[...] = rows_all - jnp.log(steps)
    to_end = jnp.exp(rows_all[:, BLOCK - 1 : BLOCK] - rows_all) * steps
    ends_ref[...] = to_end
    for k in range(blocks):
        cols_ref[k] = cols_all[:, k * padded : (k + 1) * padded]

    loads[2].wait()
    loads[3].wait()
    for load in loads[4:]:
        load.start()
    for first in range(0, len(every), 2):
        some = every[first : first + 2]

        def state_step(pair, carry, some=some):
            for k in (2 * pair, 2 * pair + 1):
                row = pl.ds(pl.multiple_of(k * BLOCK, BLOCK), BLOCK)
                spot = pl.ds(pl.multiple_of(k * 8, 8), 8)
                following = pl.ds(pl.multiple_of(k * 8 + 8, 8), 8)
                end = cols_ref[k, BLOCK - 8 : BLOCK, :][7:8, :]
                ends = ends_ref[pl.ds(pl.multiple_of(k * padded, padded), padded), :]
                turned = {}
                for p, start, width, of, group in some:
                    lanes = slice(start, start + width)
                    last = spread(end, of, width)
                    if group not in turned:
                        turned[group] = b[row, group * STATE : (group + 1) * STATE].T.astype(F32)
                    scaled = [(turned[group] * ends[head : head + 1, :]).astype(BF16) for head in of]
                    both = dot(jnp.concatenate(scaled, axis=0), x[row, lanes], 1, 0)
                    new = jnp.where(iotas(STATE, width)[1] < HEAD_DIM, both[:STATE], both[STATE:])
                    prefix[k + 1, :, lanes] = jnp.exp(last) * prefix[k, :, lanes] + new
                    base[following, lanes] = base[spot, lanes] + last
            return carry

        lax.fori_loop(0, blocks // 2, state_step, 0)

        @pl.when(z == 0)
        def _(some=some):
            for p, start, width, of, group in some:
                state_out[p, :, :width] = prefix[blocks, :, start : start + width].astype(BF16)
                state_copy(p).start()

    def pass_state():
        for p, start, width, of, group in every:
            lanes = slice(start, start + width)
            state_copy(p).wait_recv()

            @pl.when(z < S - 1)
            def _():
                grown = jnp.exp(base[blocks * 8 : blocks * 8 + 1, lanes]) * state_in[p, :, :width].astype(F32)
                state_out[p, :, :width] = (grown + prefix[blocks, :, lanes]).astype(BF16)
                state_copy(p).start()

    def block_of(j):
        mixed = j < 2 * share_blocks
        rest = j - 2 * share_blocks
        dx = jnp.where(mixed, 1 - j % 2, 1 - rest // share_blocks)
        dy = jnp.where(mixed, 1, 0)
        sub = jnp.where(mixed, j // 2, rest % share_blocks)
        return dx, dy, sub

    def within(k):
        row = pl.ds(pl.multiple_of(k * BLOCK, BLOCK), BLOCK)
        mid = BLOCK // 2
        columns = cols_ref[k]
        rows = rows_ref[pl.ds(pl.multiple_of(k * padded, padded), padded), :]
        scores = {}
        for p, start, width, of, group in every:
            lanes = slice(start, start + width)
            if group not in scores:
                which = slice(group * STATE, (group + 1) * STATE)
                scores[group] = dot(c[row, which], b[row, which], 1, 1) * lower
            x_here = x[row, lanes]
            lane = iotas(BLOCK, width)[1]
            top, bottom = 0.0, 0.0
            for i, head in enumerate(of):
                kept = (lane >= i * HEAD_DIM) & (lane < (i + 1) * HEAD_DIM)
                x_head = x_here if len(of) == 1 else jnp.where(kept, x_here, jnp.zeros_like(x_here))
                column, across = columns[:, head : head + 1], rows[head : head + 1, :]
                w_top = scores[group][:mid, :mid] * jnp.exp(
                    jnp.minimum(column[:mid] - across[:, :mid], 0.0)
                )
                w_bottom = scores[group][mid:] * jnp.exp(jnp.minimum(column[mid:] - across, 0.0))
                top = top + dot(w_top.astype(BF16), x_head[:mid], 1, 0)
                bottom = bottom + dot(w_bottom.astype(BF16), x_head, 1, 0)
            gains = jnp.full((1, width), skip_ref[of[0]], F32)
            if len(of) > 1:
                gains = jnp.where(iotas(1, width)[1] < HEAD_DIM, gains, skip_ref[of[1]])
            direct = gains * x_here.astype(F32)
            x[row, lanes] = jnp.concatenate([top + direct[:mid], bottom + direct[mid:]], axis=0).astype(BF16)

    def row_of(dx, dy, sub):
        owner = ((gy + dy) % Y) * X + (gx + dx) % X
        return pl.multiple_of(owner * per_share + sub * unit, unit)

    def copy_gated(dy, sub):
        return pltpu.make_async_remote_copy(
            src_ref=x.at[pl.ds(row_of(1, dy, sub), unit), :], dst_ref=gated_in.at[dy, sub],
            send_sem=gated_send.at[dy, sub], recv_sem=gated_recv.at[dy, sub],
            device_id=to(1, 0), device_id_type=MESH,
        )

    def copy_squares(dx, dy, sub, index):
        slot = dx * Y + dy
        return pltpu.make_async_remote_copy(
            src_ref=squares.at[index], dst_ref=squares_in.at[slot, sub],
            send_sem=square_send.at[slot, sub], recv_sem=square_recv.at[slot, sub],
            device_id=to(dx, dy), device_id_type=MESH,
        )

    def copy_sums(sub, m):
        return pltpu.make_async_remote_copy(
            src_ref=sums_out.at[sub, m], dst_ref=sums_in.at[sub, m],
            send_sem=sums_send.at[sub, m], recv_sem=sums_recv.at[sub, m],
            device_id=to(0, 1), device_id_type=MESH,
        )

    def first_row(j):
        dx, dy, part_of_share = block_of(j)
        return row_of(dx, dy, part_of_share * units)

    def finish(j):
        dx, dy, part_of_share = block_of(j)
        k = first_row(j) // BLOCK
        row = pl.ds(pl.multiple_of(k * BLOCK, BLOCK), BLOCK)
        grow_all = jnp.exp(cols_ref[k])
        before = jnp.exp(base[pl.ds(pl.multiple_of(k * 8, 8), 8), :])
        total = {}
        for p, start, width, of, group in every:
            lanes = slice(start, start + width)
            entering = prefix[k, :, lanes] + before[0:1, lanes] * state_in[p, :, :width].astype(F32)
            moved = dot(c[row, group * STATE : (group + 1) * STATE], entering.astype(BF16), 1, 0)
            across = spread(grow_all, of, width) * moved
            v = gate[row, lanes].astype(F32)
            gated = (x[row, lanes].astype(F32) + across) * (v * (0.5 + 0.5 * jnp.tanh(0.5 * v)))
            total[width] = total.get(width, 0.0) + gated * gated
            x[row, lanes] = (gated * gain_ref[pl.ds(first_gain + p, 1), :width]).astype(BF16)
        summed = jnp.zeros((8, BLOCK), F32)
        for width, value in total.items():
            for part_of in split(value, 2):
                summed = summed + dot(jnp.ones((8, width), BF16), part_of, 1, 1)
        for u in range(units):
            squares[k * units + u] = summed[:, u * unit : (u + 1) * unit]

        @pl.when(dx > 0)
        def _():
            for u in range(units):
                copy_gated(dy, part_of_share * units + u).start()

        @pl.when(dx + dy > 0)
        def _():
            for u in range(units):
                copy_squares(dx, dy, part_of_share * units + u, k * units + u).start()

    def product(row, size, m, arrived):
        columns = pl.ds(pl.multiple_of(m * wide, wide), wide)
        return dot(x[pl.ds(row, size), :], w[:, columns], 1, 0) + dot(arrived, theirs[m], 1, 0)

    loads[4].wait()
    def main_step(i, carry):
        @pl.when(i == lag)
        def _():
            loads[5].wait()

        @pl.when(i >= lag)
        def _():
            finish(i - lag)

        @pl.when(i < blocks)
        def _():
            within(first_row(i) // BLOCK)

        @pl.when((z > 0) & (i == lax.max(z * blocks // S - 1, 0)))
        def _():
            pass_state()

        relay(i)
        return carry

    lax.fori_loop(0, blocks + lag, main_step, 0)
    loads[6].wait()

    def far_tiles(sub, first, last):
        def tile(position, carry):
            m = chunk_at(position)

            @pl.when(sub == 0)
            def _():
                w_arrival(m, 1 - core).wait_recv()

            sums_out[sub, m] = product(row_of(0, 1, sub), unit, m, gated_in[1, sub]).astype(BF16)
            copy_sums(sub, m).start()
            return carry

        lax.fori_loop(first, last, tile, 0)

    def of_step(at):
        found = jnp.int32(ready[0])
        for i in range(1, subs + 1):
            found = jnp.where(at >= i, jnp.int32(ready[i]), found)
        return found

    def far_step(sub, carry):
        copy_gated(1, sub).wait_recv()
        known = of_step(sub)
        far_tiles(sub, 0, known)
        relay(blocks + lag + sub)
        fresh = of_step(sub + 1)

        def older(other, carry):
            far_tiles(other, known, fresh)
            return carry

        lax.fori_loop(0, sub + 1, older, 0)

        def ahead(i, carry):
            block, m = i // count, i % count
            columns = pl.ds(pl.multiple_of(m * wide, wide), wide)
            own_ref[block, m] = dot(x[pl.ds(row_of(0, 0, block * units), BLOCK), :], w[:, columns], 1, 0)
            return carry

        share = -(-share_blocks * count // subs)
        lax.fori_loop(sub * share, lax.min((sub + 1) * share, share_blocks * count), ahead, 0)
        return carry

    lax.fori_loop(0, subs, far_step, 0)

    def late_step(position, carry):
        relay(position, final)

        def older(other, carry):
            far_tiles(other, position, position + 1)
            return carry

        lax.fori_loop(0, subs, older, 0)
        return carry

    lax.fori_loop(ready[subs], count, late_step, 0)

    same_u = jnp.where(iotas(unit, unit)[0] == iotas(unit, unit)[1], 1.0, 0.0)

    def scale_step(sub, carry):
        summed = squares[me * subs + sub]
        for dx in range(X):
            for dy in range(Y):
                if dx + dy > 0:
                    copy_squares(dx, dy, sub, 0).wait_recv()
                    summed = summed + squares_in[dx * Y + dy, sub]
        column = dot(same_u, summed, 1, 1, HIGHEST)[:, 0:1]
        there = pl.ds(pl.multiple_of(sub * unit, unit), unit)
        scale_ref[there, :] = jnp.broadcast_to(lax.rsqrt(column / (HEAD_COUNT * HEAD_DIM) + epsilon), (unit, LANES))
        return carry

    lax.fori_loop(0, subs, scale_step, 0)

    def out_copy(block, m):
        there = pl.ds(pl.multiple_of(block * BLOCK, BLOCK), BLOCK)
        columns = pl.ds(pl.multiple_of(m * wide, wide), wide)
        return pltpu.make_async_copy(stage.at[there, columns], out_hbm.at[there, columns], out_sem.at[block, m])

    def near_tile(block, position):
        there = pl.ds(pl.multiple_of(block * BLOCK, BLOCK), BLOCK)
        m = chunk_at(position)
        columns = pl.ds(pl.multiple_of(m * wide, wide), wide)
        arrived = jnp.concatenate([gated_in[0, block * units + u] for u in range(units)], axis=0)
        value = own_ref[block, m] + dot(arrived, theirs[m], 1, 0)
        for u in range(units):
            copy_sums(block * units + u, m).wait_recv()
        value = value + jnp.concatenate([sums_in[block * units + u, m] for u in range(units)], axis=0).astype(F32)
        scale = scale_ref[there, :]
        stage[there, columns] = (value * jnp.concatenate([scale, scale], axis=1)).astype(BF16)
        out_copy(block, m).start()

    def near_step(block, carry):
        for u in range(units):
            copy_gated(0, block * units + u).wait_recv()

        def tile(position, carry):
            near_tile(block, position)
            return carry

        lax.fori_loop(0, ready[subs], tile, 0)
        return carry

    def last_step(i, carry):
        near_tile(i % share_blocks, ready[subs] + i // share_blocks)
        return carry

    lax.fori_loop(0, share_blocks, near_step, 0)
    lax.fori_loop(0, share_blocks * (count - ready[subs]), last_step, 0)

    def drain(m, carry):
        for sub in range(subs):
            copy_sums(sub, m).wait_send()
        for block in range(share_blocks):
            out_copy(block, m).wait()
        w_copy(m, "side").wait_send()
        return carry

    lax.fori_loop(0, count, drain, 0)
    for sub in range(subs):
        for dy in range(Y):
            copy_gated(dy, sub).wait_send()
        for dx in range(X):
            for dy in range(Y):
                if dx + dy > 0:
                    copy_squares(dx, dy, sub, 0).wait_send()
    for zz in range(S):
        @pl.when(z == zz)
        def _(zz=zz):
            for m in range(count):
                if homes[m] == zz:
                    w_copy(m, "first").wait_send()
                if zz > 0 and homes[m] >= zz:
                    w_copy(m, "left").wait_send()
                if zz < S - 1 and homes[m] <= zz:
                    w_copy(m, "right").wait_send()

    @pl.when(z < S - 1)
    def _():
        for p, start, width, of, group in every:
            state_copy(p).wait_send()


def body(
    ssm_input, gate_input, b_proj, c_proj, step_size, log_decay, skip_gain, norm_gain, out_weight
):
    tokens, channels = ssm_input.shape
    heads = step_size.shape[0]
    blocks = tokens // BLOCK
    model = out_weight.shape[1]
    half = model // 2
    per_group = HEAD_COUNT // GROUPS
    groups = max(1, heads // per_group)
    repeats = min(heads, per_group)
    H = lax.axis_size("head")
    S = lax.axis_size("seq")
    X = max(d for d in range(1, H + 1) if H % d == 0 and d * d <= H)
    Y = H // X
    per_share = tokens // H
    unit = min(UNIT, per_share)
    subs = per_share // unit
    count = len(pieces(channels, repeats))
    padded = -(-heads // 8) * 8
    head_index = lax.axis_index("head")
    gain = norm_gain
    if channels % LANES != 0:
        gain = lax.dynamic_slice_in_dim(norm_gain, head_index * channels, channels)
        gain = jnp.pad(gain, (0, count * LANES - channels))
    gain = gain.reshape(-1, LANES)
    anywhere = pl.BlockSpec(memory_space=pl.ANY)
    vmem = pl.BlockSpec(memory_space=pltpu.VMEM)
    dma = pltpu.SemaphoreType.DMA
    x1, y1 = max(X - 1, 1), max(Y - 1, 1)
    side = [anywhere] * 6 + [pl.BlockSpec(memory_space=pltpu.SMEM), vmem, anywhere]
    paired = (
        X == 2 and Y == 2 and S > 1 and lax.axis_size("batch") == 2 and per_share % BLOCK == 0
        and model % (2 * LANES) == 0 and channels % LANES == 0 and model // (2 * LANES) >= S
        and per_share == 4 * UNIT and blocks % 2 == 0
    )
    common = [
        pltpu.VMEM((tokens, channels), BF16),
        pltpu.VMEM((tokens, channels), BF16),
        pltpu.VMEM((tokens, groups * STATE), BF16),
        pltpu.VMEM((tokens, groups * STATE), BF16),
        pltpu.VMEM((heads, tokens), F32),
        pltpu.VMEM((heads, tokens), F32),
        pltpu.VMEM((channels, model), BF16),
        pltpu.VMEM((blocks * padded, BLOCK), F32),
        pltpu.VMEM((blocks * padded, BLOCK), F32),
        pltpu.VMEM((blocks * padded, BLOCK), F32),
        pltpu.VMEM((blocks, BLOCK, padded), F32),
        pltpu.VMEM((blocks * padded, BLOCK), F32),
        pltpu.VMEM((blocks + 1, STATE, channels), F32),
        pltpu.VMEM(((blocks + 1) * 8, channels), F32),
        pltpu.VMEM((count, STATE, LANES), BF16),
        pltpu.VMEM((count, STATE, LANES), BF16),
    ]
    cost = pl.CostEstimate(
        flops=2 * tokens * channels * (model + 4 * BLOCK), bytes_accessed=tokens * channels * 8, transcendentals=0
    )
    params = pltpu.CompilerParams(
        collective_id=0, has_side_effects=True, vmem_limit_bytes=62 * 1024 * 1024
    )
    if paired:
        tiles = model // (2 * LANES)
        return pl.pallas_call(
            functools.partial(pair_kernel, (X, Y, S, groups, repeats)),
            in_specs=side,
            out_specs=anywhere,
            out_shape=jax.ShapeDtypeStruct((per_share, model), BF16),
            scratch_shapes=common + [
                pltpu.VMEM((tiles, channels, 2 * LANES), BF16),
                pltpu.VMEM((tokens // unit, 8, unit), F32),
                pltpu.VMEM((H, subs, 8, unit), F32),
                pltpu.VMEM((Y, subs, unit, channels), BF16),
                pltpu.VMEM((subs, tiles, unit, 2 * LANES), BF16),
                pltpu.VMEM((subs, tiles, unit, 2 * LANES), BF16),
                pltpu.VMEM((per_share, model), BF16),
                pltpu.VMEM((per_share, LANES), F32),
                pltpu.VMEM((per_share // BLOCK, tiles, BLOCK, 2 * LANES), F32),
                dma((7,)),
                dma((per_share // BLOCK, tiles)),
                dma((count,)),
                dma((count,)),
                dma((H, subs)),
                dma((H, subs)),
                dma((4, tiles)),
                dma((tiles, 2)),
                dma((Y, subs)),
                dma((Y, subs)),
                dma((subs, tiles)),
                dma((subs, tiles)),
            ],
            compiler_params=params,
            name="mixer_pair",
            cost_estimate=cost,
        )(ssm_input, gate_input, b_proj, c_proj, step_size, log_decay, skip_gain, gain, out_weight)
    return pl.pallas_call(
        functools.partial(mixer_kernel, (X, Y, S, groups, repeats)),
        in_specs=side,
        out_specs=anywhere,
        out_shape=jax.ShapeDtypeStruct((per_share, model), BF16),
        scratch_shapes=common + [
            pltpu.VMEM((BLOCK, channels), BF16),
            pltpu.VMEM((tokens, model), BF16),
            pltpu.VMEM((tokens // unit, 8, unit), F32),
            pltpu.VMEM((H, subs, 8, unit), F32),
            pltpu.VMEM((x1, Y, subs, unit, half), BF16),
            pltpu.VMEM((y1, X, subs, unit, model - half), BF16),
            pltpu.VMEM((y1, subs, unit, half), BF16),
            pltpu.VMEM((x1, subs, unit, model - half), BF16),
            pltpu.VMEM((per_share, model), BF16),
            dma((7,)),
            dma((subs,)),
            dma((count,)),
            dma((count,)),
            dma((H, subs)),
            dma((H, subs)),
            dma((x1, Y, subs)),
            dma((x1, Y, subs)),
            dma((y1, X, subs)),
            dma((y1, X, subs)),
            dma((y1, subs)),
            dma((y1, subs)),
            dma((x1, subs)),
            dma((x1, subs)),
        ],
        compiler_params=params,
        name="mixer",
        cost_estimate=cost,
    )(ssm_input, gate_input, b_proj, c_proj, step_size, log_decay, skip_gain, gain, out_weight)


def solution(mesh):
    in_specs = (
        P(("batch", "seq"), "head"),
        P(("batch", "seq"), "head"),
        P(("batch", "seq"), None),
        P(("batch", "seq"), None),
        P("head", ("batch", "seq")),
        P("head", ("batch", "seq")),
        P("head"),
        P(),
        P("head", None),
    )
    out_specs = P(("batch", "seq", "head"), None)
    return jax.shard_map(body, mesh=mesh, in_specs=in_specs, out_specs=out_specs, check_vma=False)
```
